32 devices in a mesh: lat: 16 (over z, y, x), dp: 2 (over core).
Axes of the slice: x: 2, y: 2, z: 4, core: 2. Of those that a mesh axis runs over, the one named last changes fastest.
Arguments:
- state: float32 [2, 128, 256, 128], P('dp', 'lat'), may hold values from -6 to 6
- cotangent: float32 [2, 128, 256, 128], P('dp', 'lat'), may hold values from -0.18 to 0.18
- w_first: bfloat16 [128, 1024], replicated, may hold values from -0.5 to 0.5
- w_middle: bfloat16 [1024, 1024], replicated, may hold values from -0.1875 to 0.1875
- w_last: bfloat16 [1024, 128], replicated, may hold values from -0.1875 to 0.1875
Outputs:
- final_state: float32 [2, 128, 256, 128], P('dp', 'lat')
- grad_first: float32 [128, 1024], replicated
- grad_middle: float32 [1024, 1024], replicated
- grad_last: float32 [1024, 128], replicated
The draws below stay inside these ranges and needn't reach their ends.
All inputs are finite; a program needn't handle non-finite values.
Results may differ from the reference program's by a relative error of at most 0.0048.
Values sent between devices are 32-bit elements; how exact they have to be, the bound alone decides.
A program may use at most 128 MiB of HBM per device.

```python
import math
import jax
import jax.numpy as jnp
from jax import lax

NLAT = 128
NLON = 256
MW = 64
FEAT = 128
HID = 1024
STEPS = 2
BATCH = 2


def shard_levels(stream_key, dims, cuts, least, top_value):
    factor_of = 1.0
    for position, blocks in cuts:
        heights = jax.random.uniform(jax.random.fold_in(jax.random.fold_in(stream_key, 6), position), (blocks,), jnp.float32, least / len(cuts), top_value / len(cuts))
        factor_of = factor_of * jnp.repeat(jnp.exp(heights), dims[position] // blocks).reshape((-1,) + (1,) * (len(dims) - 1 - position))
    return factor_of


def bell_draw(key, dims, width, most, split=(), held_as=jnp.bfloat16):
    level = shard_levels(key, dims, split, -0.22, 0.18) if split else 1.0
    values = jax.random.normal(key, dims, jnp.float32) * width * level
    return jnp.minimum(jnp.maximum(values, -most), most).astype(held_as)


def setup_inputs(seed: int = 0) -> dict:
    seeds = jax.random.split(jax.random.key(seed), 6)
    return {
        "state": bell_draw(seeds[0], (BATCH, NLAT, NLON, FEAT), 1.0, 6.0, ((0, 2), (1, 16)), jnp.float32),
        "cotangent": bell_draw(seeds[1], (BATCH, NLAT, NLON, FEAT), 0.03, 0.18, ((0, 2), (1, 16)), jnp.float32),
        "w_first": bell_draw(seeds[2], (FEAT, HID), FEAT ** -0.5, 0.5),
        "w_middle": bell_draw(seeds[3], (HID, HID), HID ** -0.5, 0.1875),
        "w_last": bell_draw(seeds[4], (HID, FEAT), HID ** -0.5, 0.1875),
    }


highest = lax.Precision.HIGHEST
tend_weight = 0.5

def grid_tables(lon_count, wave_count):
    lon_index = jnp.arange(lon_count, dtype=jnp.int32)
    wave_index = jnp.arange(wave_count, dtype=jnp.int32)
    phase_angle = (lon_index[:, None] * wave_index[None, :] % lon_count).astype(jnp.float32) * (2.0 * math.pi / lon_count)
    cosine = jnp.cos(phase_angle)
    sine_part = jnp.sin(phase_angle)
    analysis = jnp.stack([cosine, -sine_part], axis=2) / lon_count
    factor = jnp.where(wave_index == 0, 1.0, 2.0).astype(jnp.float32)
    synthesis = jnp.stack([cosine, -sine_part], axis=2) * factor[None, :, None]
    return (analysis, synthesis)

def legendre(wave_ids, lat_count, wave_count):
    lat_index = jnp.arange(lat_count).astype(jnp.float32)
    latitude = (lat_index + 0.5) * (math.pi / lat_count) - 0.5 * math.pi
    sine_lat = jnp.sin(latitude)
    cosine_lat = jnp.cos(latitude)
    quad_weight = cosine_lat * (math.pi / lat_count)
    order_m = wave_ids.astype(jnp.float32)
    counter = jnp.arange(1, wave_count).astype(jnp.float32)
    increments = 0.5 * jnp.log((2.0 * counter + 1.0) / (2.0 * counter))
    summed = lax.optimization_barrier(jnp.sum(jnp.where(counter[None, :] <= order_m[:, None], increments[None, :], 0.0), axis=1))
    diagonal = jnp.exp(0.5 * math.log(0.5) + summed[:, None] + order_m[:, None] * jnp.log(cosine_lat)[None, :])

    def advance(carry, offset):
        previous, current, ratio_prev = carry
        degree = order_m + offset
        ratio_new = jnp.sqrt((4.0 * degree * degree - 1.0) / (degree * degree - order_m * order_m))
        following = ratio_new[:, None] * (sine_lat[None, :] * current - previous / ratio_prev[:, None])
        return ((current, following, ratio_new), following)
    initial = (jnp.zeros_like(diagonal), diagonal, jnp.ones_like(order_m))
    _, remaining = lax.scan(advance, initial, jnp.arange(1, wave_count).astype(jnp.float32))
    poly_table = jnp.concatenate([diagonal[None], remaining], axis=0).transpose(1, 0, 2)
    degree = order_m[:, None] + jnp.arange(wave_count).astype(jnp.float32)[None, :]
    kept_mask = degree <= wave_count - 1
    poly_table = jnp.where(kept_mask[:, :, None], poly_table, 0.0)
    damping = jnp.where(kept_mask, 1.0 / (1.0 + degree * (degree + 1.0) / (wave_count * (wave_count - 1.0))), 0.0)
    return (poly_table, quad_weight, damping)

def spectral_whole(field, first, last, in_table, out_table, damping):
    wave_grid = jnp.einsum('bjxf,xmp->bjmpf', field, first, precision=highest)
    coeffs = jnp.einsum('mkj,bjmpf->bmkpf', in_table, wave_grid, precision=highest) * damping[None, :, :, None, None]
    back_grid = jnp.einsum('mkj,bmkpf->bjmpf', out_table, coeffs, precision=highest)
    return jnp.einsum('bjmpf,xmp->bjxf', back_grid, last, precision=highest)

def silu_slope(value):
    gate_sig = jax.nn.sigmoid(value)
    return gate_sig * (1.0 + value * (1.0 - gate_sig))

def hidden_rows(rows, w_first, w_middle):
    pre_first = jnp.dot(rows, w_first, preferred_element_type=jnp.float32)
    hidden_first = jax.nn.silu(pre_first).astype(jnp.bfloat16)
    pre_middle = jnp.dot(hidden_first, w_middle, preferred_element_type=jnp.float32)
    hidden_middle = jax.nn.silu(pre_middle).astype(jnp.bfloat16)
    return (pre_first, hidden_first, pre_middle, hidden_middle)

def forward_rows(rows, w_first, w_middle, w_last):
    _, _, _, hidden_middle = hidden_rows(rows, w_first, w_middle)
    return jnp.dot(hidden_middle, w_last, preferred_element_type=jnp.float32)

def backward_rows(rows, scaled, w_first, w_middle, w_last):
    pre_first, hidden_first, pre_middle, hidden_middle = hidden_rows(rows, w_first, w_middle)
    grad_last = jnp.dot(hidden_middle.T, scaled, preferred_element_type=jnp.float32)
    middle_back = jnp.dot(scaled, w_last.T, preferred_element_type=jnp.float32)
    middle_grad = (middle_back * silu_slope(pre_middle)).astype(jnp.bfloat16)
    grad_middle = jnp.dot(hidden_first.T, middle_grad, preferred_element_type=jnp.float32)
    first_back = jnp.dot(middle_grad, w_middle.T, preferred_element_type=jnp.float32)
    first_grad = (first_back * silu_slope(pre_first)).astype(jnp.bfloat16)
    grad_first = jnp.dot(rows.T, first_grad, preferred_element_type=jnp.float32)
    back_rows = jnp.dot(first_grad, w_first.T, preferred_element_type=jnp.float32)
    return ((grad_first, grad_middle, grad_last), back_rows)

def reference(state, cotangent, w_first, w_middle, w_last):
    batch, lat_count, lon_count, features = state.shape
    hidden_count = w_first.shape[1]
    analysis, synthesis = grid_tables(lon_count, MW)
    poly_table, quad_weight, damping = legendre(jnp.arange(MW, dtype=jnp.int32), lat_count, MW)
    weighted = poly_table * quad_weight[None, None, :]
    row_count = batch * lat_count * lon_count
    block = math.gcd(row_count, 8192)
    inputs = []
    field = state
    for step_index in range(STEPS):
        inputs.append(field)
        rows = field.reshape(row_count // block, block, features).astype(jnp.bfloat16)
        tendency = lax.map(lambda piece: forward_rows(piece, w_first, w_middle, w_last), rows)
        moved = field + tend_weight * tendency.reshape(field.shape)
        field = spectral_whole(moved, analysis, synthesis, weighted, poly_table, damping)
    final_state = field
    grad = cotangent
    totals = (jnp.zeros((features, hidden_count), jnp.float32), jnp.zeros((hidden_count, hidden_count), jnp.float32), jnp.zeros((hidden_count, features), jnp.float32))
    for step_index in reversed(range(STEPS)):
        pulled = spectral_whole(grad, synthesis, analysis, poly_table, weighted, damping)
        scaled = (tend_weight * pulled).astype(jnp.bfloat16).reshape(row_count // block, block, features)
        rows = inputs[step_index].reshape(row_count // block, block, features).astype(jnp.bfloat16)

        def accumulate(carry, pieces):
            grads, back_rows = backward_rows(pieces[0], pieces[1], w_first, w_middle, w_last)
            return ((carry[0] + grads[0], carry[1] + grads[1], carry[2] + grads[2]), back_rows)
        totals, back_rows = lax.scan(accumulate, totals, (rows, scaled))
        grad = pulled + back_rows.reshape(field.shape)
    return (final_state, totals[0], totals[1], totals[2])
```

```python
import functools
import math

import jax
import jax.numpy as jnp
import numpy as np
from jax import lax
from jax.experimental import pallas as pl
from jax.experimental.pallas import tpu as pltpu
from jax.sharding import PartitionSpec as P

MW = 64
STEPS = 2

high = lax.Precision.HIGH
tend_weight = 0.5


def grid_tables(lon_count, wave_count):
    lon_index = np.arange(lon_count)
    wave_index = np.arange(wave_count)
    angle = 2.0 * math.pi * (lon_index[:, None] * wave_index[None, :] % lon_count) / lon_count
    pair = np.stack([np.cos(angle), -np.sin(angle)], axis=2)
    factor = np.where(wave_index == 0, 1.0, 2.0)
    analysis = (pair / lon_count).reshape(lon_count, -1).astype(np.float32)
    synthesis = (pair * factor[None, :, None]).reshape(lon_count, -1).astype(np.float32)
    return analysis, synthesis


def legendre_tables(lat_count, wave_count):
    latitude = -0.5 * math.pi + (np.arange(lat_count) + 0.5) * math.pi / lat_count
    mu, cosine = np.sin(latitude), np.cos(latitude)
    quad_weight = cosine * math.pi / lat_count
    order = np.arange(wave_count, dtype=np.float64)
    steps = np.concatenate([[0.0], 0.5 * np.log((2 * order[1:] + 1) / (2 * order[1:]))])
    diagonal = np.exp(
        0.5 * math.log(0.5) + np.cumsum(steps)[:, None] + order[:, None] * np.log(cosine)[None, :]
    )
    rows = [diagonal]
    previous, current, ratio_prev = np.zeros_like(diagonal), diagonal, np.ones_like(order)
    for offset in range(1, wave_count):
        n = order + offset
        ratio = np.sqrt((4 * n * n - 1) / (n * n - order * order))
        following = ratio[:, None] * (mu[None, :] * current - previous / ratio_prev[:, None])
        previous, current, ratio_prev = current, following, ratio
        rows.append(following)
    table = np.stack(rows, axis=1)
    degree = order[:, None] + np.arange(wave_count)[None, :]
    kept = degree <= wave_count - 1
    damping = np.where(kept, 1.0 / (1.0 + degree * (degree + 1) / (wave_count * (wave_count - 1.0))), 0.0)
    table = np.where(kept[:, :, None], table, 0.0) * np.sqrt(damping)[:, :, None]
    return table.astype(np.float32), quad_weight.astype(np.float32)


def silu_pair(value):
    gate = 0.5 * jnp.tanh(0.5 * value) + 0.5
    hidden = value * gate
    return hidden, gate + hidden - hidden * gate


def forward_kernel(x_ref, w1_ref, w2_ref, w3_ref, moved_ref, h1_ref, s1_ref, h2_ref, s2_ref):
    field = x_ref[...]
    rows = field.astype(jnp.bfloat16)
    h1, s1 = silu_pair(jnp.dot(rows, w1_ref[...], preferred_element_type=jnp.float32))
    h1 = h1.astype(jnp.bfloat16)
    h1_ref[...] = h1
    s1_ref[...] = s1.astype(jnp.bfloat16)
    h2, s2 = silu_pair(jnp.dot(h1, w2_ref[...], preferred_element_type=jnp.float32))
    h2 = h2.astype(jnp.bfloat16)
    h2_ref[...] = h2
    s2_ref[...] = s2.astype(jnp.bfloat16)
    tend = jnp.dot(h2, w3_ref[...], preferred_element_type=jnp.float32)
    moved_ref[...] = field + tend_weight * tend


def forward_rows(x, w1, w2, w3):
    count, features = x.shape
    hidden = w1.shape[1]
    tile = math.gcd(count, 256)
    row = lambda width: pl.BlockSpec((tile, width), lambda i: (i, 0))
    whole = lambda w: pl.BlockSpec(w.shape, lambda i: (0, 0))
    wide = jax.ShapeDtypeStruct((count, hidden), jnp.bfloat16)
    return pl.pallas_call(
        forward_kernel,
        grid=(count // tile,),
        in_specs=[row(features), whole(w1), whole(w2), whole(w3)],
        out_specs=[row(features)] + [row(hidden)] * 4,
        out_shape=[jax.ShapeDtypeStruct(x.shape, jnp.float32)] + [wide] * 4,
        cost_estimate=pl.CostEstimate(
            flops=2 * count * (2 * features * hidden + hidden * hidden),
            bytes_accessed=count * hidden * 8, transcendentals=2 * count * hidden,
        ),
        compiler_params=pltpu.CompilerParams(dimension_semantics=("arbitrary",)),
    )(x, w1, w2, w3)


def mul_t(a, b):
    return lax.dot_general(a, b, (((1,), (1,)), ((), ())), preferred_element_type=jnp.float32)


def t_mul(a, b):
    return lax.dot_general(a, b, (((0,), (0,)), ((), ())), preferred_element_type=jnp.float32)


def backward_kernel(first_call, need_rows, *refs):
    p_ref, x_ref, h1_ref, s1_ref, h2_ref, s2_ref, w1_ref, w2_ref, w3_ref = refs[:9]
    refs = refs[9:]
    if not first_call:
        c1_ref, c2_ref, c3_ref = refs[:3]
        refs = refs[3:]
    g1_ref, g2_ref, g3_ref = refs[:3]

    @pl.when(pl.program_id(0) == 0)
    def _():
        if first_call:
            g1_ref[...] = jnp.zeros_like(g1_ref)
            g2_ref[...] = jnp.zeros_like(g2_ref)
            g3_ref[...] = jnp.zeros_like(g3_ref)
        else:
            g1_ref[...] = c1_ref[...]
            g2_ref[...] = c2_ref[...]
            g3_ref[...] = c3_ref[...]

    pulled = p_ref[...]
    gt = (tend_weight * pulled).astype(jnp.bfloat16)
    g3_ref[...] += t_mul(h2_ref[...], gt)
    ga2 = (mul_t(gt, w3_ref[...]) * s2_ref[...].astype(jnp.float32)).astype(jnp.bfloat16)
    g2_ref[...] += t_mul(h1_ref[...], ga2)
    ga1 = (mul_t(ga2, w2_ref[...]) * s1_ref[...].astype(jnp.float32)).astype(jnp.bfloat16)
    g1_ref[...] += t_mul(x_ref[...].astype(jnp.bfloat16), ga1)
    if need_rows:
        refs[3][...] = pulled + mul_t(ga1, w1_ref[...])


def backward_rows(pulled, x, saved, w1, w2, w3, carry, need_rows):
    count, features = x.shape
    hidden = w1.shape[1]
    tile = math.gcd(count, 512)
    row = lambda width: pl.BlockSpec((tile, width), lambda i: (i, 0))
    whole = lambda w: pl.BlockSpec(w.shape, lambda i: (0, 0))
    out_shape = [jax.ShapeDtypeStruct(w.shape, jnp.float32) for w in (w1, w2, w3)]
    out_specs = [whole(w) for w in (w1, w2, w3)]
    carried = [] if carry is None else list(carry)
    if need_rows:
        out_shape.append(jax.ShapeDtypeStruct(x.shape, jnp.float32))
        out_specs.append(row(features))
    return pl.pallas_call(
        functools.partial(backward_kernel, carry is None, need_rows),
        grid=(count // tile,),
        in_specs=[row(features)] * 2 + [row(hidden)] * 4
        + [whole(w) for w in (w1, w2, w3)] + [whole(c) for c in carried],
        out_specs=out_specs,
        out_shape=out_shape,
        cost_estimate=pl.CostEstimate(
            flops=4 * count * (2 * features * hidden + hidden * hidden),
            bytes_accessed=count * hidden * 8, transcendentals=0,
        ),
        compiler_params=pltpu.CompilerParams(dimension_semantics=("arbitrary",)),
    )(pulled, x, *saved, w1, w2, w3, *carried)


MESH_ID = pl.DeviceIdType.MESH
LANES = 128
CHUNK = 1024


class Place:
    def __init__(self, bands):
        self.me = lax.axis_index("lat")
        self.core = lax.axis_index("dp")
        self.depth = bands // 4
        self.x = lax.rem(self.me, 2)
        self.y = lax.rem(self.me // 2, 2)
        self.z = self.me // 4
        self.across_core = {"dp": 1 - self.core}
        self.across_x = {"lat": self.me + 1 - 2 * self.x}
        self.across_y = {"lat": self.me + 2 - 4 * self.y}

    def along_z(self, step):
        layer = lax.rem(self.z + step, self.depth)
        return layer, {"lat": layer * 4 + lax.rem(self.me, 4)}


def signal_to(device):
    pl.semaphore_signal(pltpu.get_barrier_semaphore(), inc=1, device_id=device, device_id_type=MESH_ID)


def greet_reduce(place):
    signal_to(place.across_core)
    signal_to(place.across_x)
    signal_to(place.across_y)
    for step in range(1, place.depth):
        signal_to(place.along_z(step)[1])
    pl.semaphore_wait(pltpu.get_barrier_semaphore(), place.depth + 2)


def send(src, dst, ssem, rsem, device):
    pltpu.make_async_remote_copy(
        src_ref=src, dst_ref=dst, send_sem=ssem, recv_sem=rsem, device_id=device, device_id_type=MESH_ID
    ).start()


def wait_bytes(ref, sem):
    pltpu.make_async_copy(ref, ref, sem).wait()


class Reduce:
    SENDS = 8

    @staticmethod
    def scratch(chunks, depth):
        rows = lambda count: pltpu.VMEM((chunks * count, LANES), jnp.float32)
        sems = lambda *dims: pltpu.SemaphoreType.DMA((chunks,) + dims)
        return [
            rows(CHUNK), rows(CHUNK), rows(512), rows(256), rows(128),
            pltpu.VMEM((chunks, depth - 1, 256 // depth // 2, LANES), jnp.float32),
            sems(), sems(2), sems(2), sems(depth - 1), sems(depth - 1), sems(2), sems(2), sems(),
            pltpu.SemaphoreType.DMA((Reduce.SENDS,)),
        ]

    def __init__(self, place, chunks, refs):
        (self.g, self.o, self.r0, self.r1, self.r2, self.r3,
         self.d0, self.m1, self.m2, self.z3, self.z4, self.m5, self.m6, self.d7, self.sent) = refs
        self.place, self.chunks = place, chunks
        self.piece = 64 // place.depth
        p = place
        half = p.core * 512
        self.first = ((p.across_x, p.x), (p.across_y, p.y))
        self.second = (self.first[1], self.first[0])
        self.quarter = (half, half + 256)
        self.eighth = tuple(self.quarter[i] + self.first[i][1] * 128 for i in (0, 1))
        self.sixteenth = tuple(self.eighth[i] + self.second[i][1] * 64 for i in (0, 1))
        self.own = tuple(self.sixteenth[i] + p.z * self.piece for i in (0, 1))

    def rows(self, ref, k, offset, count, span=CHUNK):
        return ref.at[pl.ds(pl.multiple_of(k * span + offset, 8), count), :]

    def stage0(self, k):
        other = (1 - self.place.core) * 512
        send(self.rows(self.g, k, other, 512), self.rows(self.r0, k, 0, 512, 512),
             self.sent.at[0], self.d0.at[k], self.place.across_core)

    def stage1(self, k):
        wait_bytes(self.rows(self.r0, k, 0, 512, 512), self.d0.at[k])
        mine = self.rows(self.g, k, self.place.core * 512, 512)
        mine[...] += self.rows(self.r0, k, 0, 512, 512)[...]
        for i in (0, 1):
            device, bit = self.first[i]
            send(self.rows(self.g, k, self.quarter[i] + (1 - bit) * 128, 128),
                 self.rows(self.r1, k, i * 128, 128, 256), self.sent.at[1], self.m1.at[k, i], device)

    def stage2(self, k):
        for i in (0, 1):
            got = self.rows(self.r1, k, i * 128, 128, 256)
            wait_bytes(got, self.m1.at[k, i])
            self.rows(self.g, k, self.eighth[i], 128)[...] += got[...]
        for i in (0, 1):
            device, bit = self.second[i]
            send(self.rows(self.g, k, self.eighth[i] + (1 - bit) * 64, 64),
                 self.rows(self.r2, k, i * 64, 64, 128), self.sent.at[2], self.m2.at[k, i], device)

    def stage3(self, k):
        for i in (0, 1):
            got = self.rows(self.r2, k, i * 64, 64, 128)
            wait_bytes(got, self.m2.at[k, i])
            self.rows(self.g, k, self.sixteenth[i], 64)[...] += got[...]
        for step in range(1, self.place.depth):
            layer, device = self.place.along_z(step)
            for i in (0, 1):
                send(self.rows(self.g, k, self.sixteenth[i] + layer * self.piece, self.piece),
                     self.r3.at[k, step - 1, pl.ds(i * self.piece, self.piece), :],
                     self.sent.at[3], self.z3.at[k, step - 1], device)

    def stage4(self, k):
        total = [self.rows(self.g, k, self.own[i], self.piece)[...] for i in (0, 1)]
        for step in range(1, self.place.depth):
            wait_bytes(self.r3.at[k, step - 1], self.z3.at[k, step - 1])
            for i in (0, 1):
                total[i] += self.r3[k, step - 1, pl.ds(i * self.piece, self.piece), :]
        for i in (0, 1):
            self.rows(self.o, k, self.own[i], self.piece)[...] = total[i]
        for step in range(1, self.place.depth):
            _, device = self.place.along_z(step)
            for i in (0, 1):
                mine = self.rows(self.o, k, self.own[i], self.piece)
                send(mine, mine, self.sent.at[4], self.z4.at[k, step - 1], device)

    def stage5(self, k):
        for step in range(1, self.place.depth):
            wait_bytes(self.r3.at[k, step - 1], self.z4.at[k, step - 1])
        for i in (0, 1):
            mine = self.rows(self.o, k, self.sixteenth[i], 64)
            send(mine, mine, self.sent.at[5], self.m5.at[k, i], self.second[i][0])

    def stage6(self, k):
        for i in (0, 1):
            wait_bytes(self.rows(self.r2, k, 0, 64, 128), self.m5.at[k, i])
        for i in (0, 1):
            mine = self.rows(self.o, k, self.eighth[i], 128)
            send(mine, mine, self.sent.at[6], self.m6.at[k, i], self.first[i][0])

    def stage7(self, k):
        for i in (0, 1):
            wait_bytes(self.rows(self.r1, k, 0, 128, 256), self.m6.at[k, i])
        mine = self.rows(self.o, k, self.place.core * 512, 512)
        send(mine, mine, self.sent.at[7], self.d7.at[k], self.place.across_core)

    def stage8(self, k):
        wait_bytes(self.rows(self.r0, k, 0, 512, 512), self.d7.at[k])

    def step(self, t):
        stages = [self.stage0, self.stage1, self.stage2, self.stage3, self.stage4,
                  self.stage5, self.stage6, self.stage7, self.stage8]
        for lag in range(8, -1, -1):
            k = t - lag

            @pl.when(jnp.logical_and(k >= 0, k < self.chunks))
            def _(k=k, lag=lag):
                stages[lag](k)

    @property
    def steps(self):
        return self.chunks + 8

    def drain(self):
        counts = [512, 256, 128, 2 * self.piece * (self.place.depth - 1)]
        counts = counts + counts[::-1]
        for i, count in enumerate(counts):
            wait_bytes(self.g.at[pl.ds(0, count * self.chunks), :], self.sent.at[i])


def reduce_kernel(bands, g1_ref, g2_ref, g3_ref, o1_ref, o2_ref, o3_ref, *scratch):
    place = Place(bands)
    hidden = g2_ref.shape[1]
    blocks = hidden // LANES
    chunks = blocks + 2
    red = Reduce(place, chunks, scratch)
    greet_reduce(place)

    for b in range(blocks):
        red.g[pl.ds(b * CHUNK, CHUNK), :] = g2_ref[:, pl.ds(b * LANES, LANES)]
        red.g[pl.ds((blocks + 1) * CHUNK + b * LANES, LANES), :] = g1_ref[:, pl.ds(b * LANES, LANES)]
    red.g[pl.ds(blocks * CHUNK, CHUNK), :] = g3_ref[...]

    @pl.loop(0, red.steps)
    def _(t):
        red.step(t)

    for b in range(blocks):
        o2_ref[:, pl.ds(b * LANES, LANES)] = red.o[pl.ds(b * CHUNK, CHUNK), :]
        o1_ref[:, pl.ds(b * LANES, LANES)] = red.o[pl.ds((blocks + 1) * CHUNK + b * LANES, LANES), :]
    o3_ref[...] = red.o[pl.ds(blocks * CHUNK, CHUNK), :]
    red.drain()


def fits_reduce(bands, pairs, features, hidden):
    return pairs == 2 and bands % 8 == 0 and bands <= 32 and features == LANES and hidden == CHUNK


def reduce_totals(totals):
    bands, pairs = lax.axis_size("lat"), lax.axis_size("dp")
    features, hidden = totals[0].shape
    if not fits_reduce(bands, pairs, features, hidden):
        return lax.psum(tuple(totals), ("lat", "dp"))
    vmem = pl.BlockSpec(memory_space=pltpu.VMEM)
    return pl.pallas_call(
        functools.partial(reduce_kernel, bands),
        in_specs=[vmem] * 3,
        out_specs=[vmem] * 3,
        out_shape=[jax.ShapeDtypeStruct(t.shape, t.dtype) for t in totals],
        scratch_shapes=Reduce.scratch(hidden // LANES + 2, bands // 4),
        compiler_params=pltpu.CompilerParams(
            collective_id=3, has_side_effects=True, vmem_limit_bytes=56 * 2**20
        ),
    )(*totals)


def body(state, cotangent, w1, w2, w3):
    sample, lat_rows, lon_count, features = state.shape
    bands = lax.axis_size("lat")
    lat_count = lat_rows * bands
    waves = MW // bands
    analysis, synthesis = grid_tables(lon_count, MW)
    table, quad = legendre_tables(lat_count, MW)
    mine = lax.dynamic_slice_in_dim(jnp.asarray(table), lax.axis_index("lat") * waves, waves, axis=0)
    base = jnp.einsum("mki,mkj->mij", mine, mine, precision=lax.Precision.HIGHEST)
    quad = jnp.asarray(quad)
    forward_op = base * quad[None, None, :]
    backward_op = base * quad[None, :, None]

    def spectral(parts):
        sent = []
        for field, first, _, _ in parts:
            wav = jnp.einsum("bjxf,xq->bqjf", field, first, precision=high)
            sent.append(wav.reshape(sample, bands, waves * 2, lat_rows, features))
        sent = jnp.concatenate(sent, axis=0).transpose(1, 0, 2, 3, 4)
        got = lax.all_to_all(sent, "lat", split_axis=0, concat_axis=0, tiled=True)
        got = got.reshape(bands, len(parts), sample, waves, 2, lat_rows, features)
        ops = jnp.stack([p[2] for p in parts]).reshape(len(parts), waves, bands, lat_rows, lat_count)
        got = got.transpose(1, 3, 0, 5, 2, 4, 6).reshape(len(parts), waves, lat_count, -1)
        ops = ops.reshape(len(parts), waves, lat_count, lat_count)
        back = jnp.einsum("smij,smjv->smiv", ops, got, precision=high)
        back = back.reshape(len(parts), waves, bands, lat_rows, sample, 2, features)
        back = back.transpose(2, 0, 4, 1, 5, 3, 6)
        back = lax.all_to_all(back, "lat", split_axis=0, concat_axis=0, tiled=True)
        out = []
        for index, (_, _, _, last) in enumerate(parts):
            piece = back[:, index].transpose(1, 0, 2, 3, 4, 5)
            piece = piece.reshape(sample, MW * 2, lat_rows, features)
            out.append(jnp.einsum("bqjf,xq->bjxf", piece, last, precision=high))
        return out

    flat = lambda field: field.reshape(sample * lat_rows * lon_count, features)
    x0 = flat(state)
    moved0, *saved0 = forward_rows(x0, w1, w2, w3)
    (pulled1,) = spectral([(cotangent, synthesis, backward_op, analysis)])
    (q1,) = spectral([(moved0.reshape(state.shape), analysis, forward_op, synthesis)])
    x1 = flat(q1)
    moved1, *saved1 = forward_rows(x1, w1, w2, w3)
    *totals, grad = backward_rows(flat(pulled1), x1, saved1, w1, w2, w3, None, True)
    (final,) = spectral([(moved1.reshape(state.shape), analysis, forward_op, synthesis)])
    (pulled0,) = spectral([(grad.reshape(state.shape), synthesis, backward_op, analysis)])
    totals = backward_rows(flat(pulled0), x0, saved0, w1, w2, w3, totals, False)
    totals = reduce_totals(totals)
    return (final, *totals)


def solution(mesh):
    field = P("dp", "lat", None, None)
    return jax.shard_map(
        body, mesh=mesh, in_specs=(field, field, P(), P(), P()),
        out_specs=(field, P(), P(), P()), check_vma=False,
    )
```

```python
import functools
import math

import jax
import jax.numpy as jnp
import numpy as np
from jax import lax
from jax.experimental import pallas as pl
from jax.experimental.pallas import tpu as pltpu
from jax.sharding import PartitionSpec as P

MW = 64
STEPS = 2

high = lax.Precision.HIGH
tend_weight = 0.5


def grid_tables(lon_count, wave_count):
    lon_index = np.arange(lon_count)
    wave_index = np.arange(wave_count)
    angle = 2.0 * math.pi * (lon_index[:, None] * wave_index[None, :] % lon_count) / lon_count
    pair = np.stack([np.cos(angle), -np.sin(angle)], axis=2)
    factor = np.where(wave_index == 0, 1.0, 2.0)
    analysis = (pair / lon_count).reshape(lon_count, -1).astype(np.float32)
    synthesis = (pair * factor[None, :, None]).reshape(lon_count, -1).astype(np.float32)
    return analysis, synthesis


def legendre_tables(lat_count, wave_count):
    latitude = -0.5 * math.pi + (np.arange(lat_count) + 0.5) * math.pi / lat_count
    mu, cosine = np.sin(latitude), np.cos(latitude)
    quad_weight = cosine * math.pi / lat_count
    order = np.arange(wave_count, dtype=np.float64)
    steps = np.concatenate([[0.0], 0.5 * np.log((2 * order[1:] + 1) / (2 * order[1:]))])
    diagonal = np.exp(
        0.5 * math.log(0.5) + np.cumsum(steps)[:, None] + order[:, None] * np.log(cosine)[None, :]
    )
    rows = [diagonal]
    previous, current, ratio_prev = np.zeros_like(diagonal), diagonal, np.ones_like(order)
    for offset in range(1, wave_count):
        n = order + offset
        ratio = np.sqrt((4 * n * n - 1) / (n * n - order * order))
        following = ratio[:, None] * (mu[None, :] * current - previous / ratio_prev[:, None])
        previous, current, ratio_prev = current, following, ratio
        rows.append(following)
    table = np.stack(rows, axis=1)
    degree = order[:, None] + np.arange(wave_count)[None, :]
    kept = degree <= wave_count - 1
    damping = np.where(kept, 1.0 / (1.0 + degree * (degree + 1) / (wave_count * (wave_count - 1.0))), 0.0)
    table = np.where(kept[:, :, None], table, 0.0) * np.sqrt(damping)[:, :, None]
    return table.astype(np.float32), quad_weight.astype(np.float32)


def silu_pair(value):
    gate = 0.5 * jnp.tanh(0.5 * value) + 0.5
    hidden = value * gate
    return hidden, gate + hidden - hidden * gate


def forward_kernel(x_ref, w1_ref, w2_ref, w3_ref, moved_ref, h1_ref, s1_ref, h2_ref, s2_ref):
    field = x_ref[...]
    rows = field.astype(jnp.bfloat16)
    h1, s1 = silu_pair(jnp.dot(rows, w1_ref[...], preferred_element_type=jnp.float32))
    h1 = h1.astype(jnp.bfloat16)
    h1_ref[...] = h1
    s1_ref[...] = s1.astype(jnp.bfloat16)
    h2, s2 = silu_pair(jnp.dot(h1, w2_ref[...], preferred_element_type=jnp.float32))
    h2 = h2.astype(jnp.bfloat16)
    h2_ref[...] = h2
    s2_ref[...] = s2.astype(jnp.bfloat16)
    tend = jnp.dot(h2, w3_ref[...], preferred_element_type=jnp.float32)
    moved_ref[...] = field + tend_weight * tend


def forward_rows(x, w1, w2, w3):
    count, features = x.shape
    hidden = w1.shape[1]
    tile = math.gcd(count, 256)
    row = lambda width: pl.BlockSpec((tile, width), lambda i: (i, 0))
    whole = lambda w: pl.BlockSpec(w.shape, lambda i: (0, 0))
    wide = jax.ShapeDtypeStruct((count, hidden), jnp.bfloat16)
    return pl.pallas_call(
        forward_kernel,
        grid=(count // tile,),
        in_specs=[row(features), whole(w1), whole(w2), whole(w3)],
        out_specs=[row(features)] + [row(hidden)] * 4,
        out_shape=[jax.ShapeDtypeStruct(x.shape, jnp.float32)] + [wide] * 4,
        cost_estimate=pl.CostEstimate(
            flops=2 * count * (2 * features * hidden + hidden * hidden),
            bytes_accessed=count * hidden * 8, transcendentals=2 * count * hidden,
        ),
        compiler_params=pltpu.CompilerParams(dimension_semantics=("arbitrary",)),
    )(x, w1, w2, w3)


def mul_t(a, b):
    return lax.dot_general(a, b, (((1,), (1,)), ((), ())), preferred_element_type=jnp.float32)


def t_mul(a, b):
    return lax.dot_general(a, b, (((0,), (0,)), ((), ())), preferred_element_type=jnp.float32)


def backward_kernel(first_call, need_rows, *refs):
    p_ref, x_ref, h1_ref, s1_ref, h2_ref, s2_ref, w1_ref, w2_ref, w3_ref = refs[:9]
    refs = refs[9:]
    if not first_call:
        c1_ref, c2_ref, c3_ref = refs[:3]
        refs = refs[3:]
    g1_ref, g2_ref, g3_ref = refs[:3]

    @pl.when(pl.program_id(0) == 0)
    def _():
        if first_call:
            g1_ref[...] = jnp.zeros_like(g1_ref)
            g2_ref[...] = jnp.zeros_like(g2_ref)
            g3_ref[...] = jnp.zeros_like(g3_ref)
        else:
            g1_ref[...] = c1_ref[...]
            g2_ref[...] = c2_ref[...]
            g3_ref[...] = c3_ref[...]

    pulled = p_ref[...]
    gt = (tend_weight * pulled).astype(jnp.bfloat16)
    g3_ref[...] += t_mul(h2_ref[...], gt)
    ga2 = (mul_t(gt, w3_ref[...]) * s2_ref[...].astype(jnp.float32)).astype(jnp.bfloat16)
    g2_ref[...] += t_mul(h1_ref[...], ga2)
    ga1 = (mul_t(ga2, w2_ref[...]) * s1_ref[...].astype(jnp.float32)).astype(jnp.bfloat16)
    g1_ref[...] += t_mul(x_ref[...].astype(jnp.bfloat16), ga1)
    if need_rows:
        refs[3][...] = pulled + mul_t(ga1, w1_ref[...])


def backward_rows(pulled, x, saved, w1, w2, w3, carry, need_rows):
    count, features = x.shape
    hidden = w1.shape[1]
    tile = math.gcd(count, 512)
    row = lambda width: pl.BlockSpec((tile, width), lambda i: (i, 0))
    whole = lambda w: pl.BlockSpec(w.shape, lambda i: (0, 0))
    out_shape = [jax.ShapeDtypeStruct(w.shape, jnp.float32) for w in (w1, w2, w3)]
    out_specs = [whole(w) for w in (w1, w2, w3)]
    carried = [] if carry is None else list(carry)
    if need_rows:
        out_shape.append(jax.ShapeDtypeStruct(x.shape, jnp.float32))
        out_specs.append(row(features))
    return pl.pallas_call(
        functools.partial(backward_kernel, carry is None, need_rows),
        grid=(count // tile,),
        in_specs=[row(features)] * 2 + [row(hidden)] * 4
        + [whole(w) for w in (w1, w2, w3)] + [whole(c) for c in carried],
        out_specs=out_specs,
        out_shape=out_shape,
        cost_estimate=pl.CostEstimate(
            flops=4 * count * (2 * features * hidden + hidden * hidden),
            bytes_accessed=count * hidden * 8, transcendentals=0,
        ),
        compiler_params=pltpu.CompilerParams(dimension_semantics=("arbitrary",)),
    )(pulled, x, *saved, w1, w2, w3, *carried)


MESH_ID = pl.DeviceIdType.MESH
LANES = 128
CHUNK = 1024


class Place:
    def __init__(self, bands):
        self.me = lax.axis_index("lat")
        self.core = lax.axis_index("dp")
        self.depth = bands // 4
        self.x = lax.rem(self.me, 2)
        self.y = lax.rem(self.me // 2, 2)
        self.z = self.me // 4
        self.across_core = {"dp": 1 - self.core}
        self.across_x = {"lat": self.me + 1 - 2 * self.x}
        self.across_y = {"lat": self.me + 2 - 4 * self.y}

    def along_z(self, step):
        layer = lax.rem(self.z + step, self.depth)
        return layer, {"lat": layer * 4 + lax.rem(self.me, 4)}


def signal_to(device):
    pl.semaphore_signal(pltpu.get_barrier_semaphore(), inc=1, device_id=device, device_id_type=MESH_ID)


def greet_reduce(place):
    signal_to(place.across_core)
    signal_to(place.across_x)
    signal_to(place.across_y)
    for step in range(1, place.depth):
        signal_to(place.along_z(step)[1])
    pl.semaphore_wait(pltpu.get_barrier_semaphore(), place.depth + 2)


def send(src, dst, ssem, rsem, device):
    pltpu.make_async_remote_copy(
        src_ref=src, dst_ref=dst, send_sem=ssem, recv_sem=rsem, device_id=device, device_id_type=MESH_ID
    ).start()


def wait_bytes(ref, sem):
    pltpu.make_async_copy(ref, ref, sem).wait()


class Reduce:
    SENDS = 8

    @staticmethod
    def scratch(chunks, depth):
        rows = lambda count: pltpu.VMEM((chunks * count, LANES), jnp.float32)
        sems = lambda *dims: pltpu.SemaphoreType.DMA((chunks,) + dims)
        return [
            rows(CHUNK), rows(CHUNK), rows(512), rows(256), rows(128),
            pltpu.VMEM((chunks, depth - 1, 256 // depth // 2, LANES), jnp.float32),
            sems(), sems(2), sems(2), sems(depth - 1), sems(depth - 1), sems(2), sems(2), sems(),
            pltpu.SemaphoreType.DMA((Reduce.SENDS,)),
        ]

    def __init__(self, place, chunks, refs):
        (self.g, self.o, self.r0, self.r1, self.r2, self.r3,
         self.d0, self.m1, self.m2, self.z3, self.z4, self.m5, self.m6, self.d7, self.sent) = refs
        self.place, self.chunks = place, chunks
        self.piece = 64 // place.depth
        p = place
        half = p.core * 512
        self.first = ((p.across_x, p.x), (p.across_y, p.y))
        self.second = (self.first[1], self.first[0])
        self.quarter = (half, half + 256)
        self.eighth = tuple(self.quarter[i] + self.first[i][1] * 128 for i in (0, 1))
        self.sixteenth = tuple(self.eighth[i] + self.second[i][1] * 64 for i in (0, 1))
        self.own = tuple(self.sixteenth[i] + p.z * self.piece for i in (0, 1))

    def rows(self, ref, k, offset, count, span=CHUNK):
        return ref.at[pl.ds(pl.multiple_of(k * span + offset, 8), count), :]

    def stage0(self, k):
        other = (1 - self.place.core) * 512
        send(self.rows(self.g, k, other, 512), self.rows(self.r0, k, 0, 512, 512),
             self.sent.at[0], self.d0.at[k], self.place.across_core)

    def stage1(self, k):
        wait_bytes(self.rows(self.r0, k, 0, 512, 512), self.d0.at[k])
        mine = self.rows(self.g, k, self.place.core * 512, 512)
        mine[...] += self.rows(self.r0, k, 0, 512, 512)[...]
        for i in (0, 1):
            device, bit = self.first[i]
            send(self.rows(self.g, k, self.quarter[i] + (1 - bit) * 128, 128),
                 self.rows(self.r1, k, i * 128, 128, 256), self.sent.at[1], self.m1.at[k, i], device)

    def stage2(self, k):
        for i in (0, 1):
            got = self.rows(self.r1, k, i * 128, 128, 256)
            wait_bytes(got, self.m1.at[k, i])
            self.rows(self.g, k, self.eighth[i], 128)[...] += got[...]
        for i in (0, 1):
            device, bit = self.second[i]
            send(self.rows(self.g, k, self.eighth[i] + (1 - bit) * 64, 64),
                 self.rows(self.r2, k, i * 64, 64, 128), self.sent.at[2], self.m2.at[k, i], device)

    def stage3(self, k):
        for i in (0, 1):
            got = self.rows(self.r2, k, i * 64, 64, 128)
            wait_bytes(got, self.m2.at[k, i])
            self.rows(self.g, k, self.sixteenth[i], 64)[...] += got[...]
        for step in range(1, self.place.depth):
            layer, device = self.place.along_z(step)
            for i in (0, 1):
                send(self.rows(self.g, k, self.sixteenth[i] + layer * self.piece, self.piece),
                     self.r3.at[k, step - 1, pl.ds(i * self.piece, self.piece), :],
                     self.sent.at[3], self.z3.at[k, step - 1], device)

    def stage4(self, k):
        total = [self.rows(self.g, k, self.own[i], self.piece)[...] for i in (0, 1)]
        for step in range(1, self.place.depth):
            wait_bytes(self.r3.at[k, step - 1], self.z3.at[k, step - 1])
            for i in (0, 1):
                total[i] += self.r3[k, step - 1, pl.ds(i * self.piece, self.piece), :]
        for i in (0, 1):
            self.rows(self.o, k, self.own[i], self.piece)[...] = total[i]
        for step in range(1, self.place.depth):
            _, device = self.place.along_z(step)
            for i in (0, 1):
                mine = self.rows(self.o, k, self.own[i], self.piece)
                send(mine, mine, self.sent.at[4], self.z4.at[k, step - 1], device)

    def stage5(self, k):
        for step in range(1, self.place.depth):
            wait_bytes(self.r3.at[k, step - 1], self.z4.at[k, step - 1])
        for i in (0, 1):
            mine = self.rows(self.o, k, self.sixteenth[i], 64)
            send(mine, mine, self.sent.at[5], self.m5.at[k, i], self.second[i][0])

    def stage6(self, k):
        for i in (0, 1):
            wait_bytes(self.rows(self.r2, k, 0, 64, 128), self.m5.at[k, i])
        for i in (0, 1):
            mine = self.rows(self.o, k, self.eighth[i], 128)
            send(mine, mine, self.sent.at[6], self.m6.at[k, i], self.first[i][0])

    def stage7(self, k):
        for i in (0, 1):
            wait_bytes(self.rows(self.r1, k, 0, 128, 256), self.m6.at[k, i])
        mine = self.rows(self.o, k, self.place.core * 512, 512)
        send(mine, mine, self.sent.at[7], self.d7.at[k], self.place.across_core)

    def stage8(self, k):
        wait_bytes(self.rows(self.r0, k, 0, 512, 512), self.d7.at[k])

    def step(self, t):
        stages = [self.stage0, self.stage1, self.stage2, self.stage3, self.stage4,
                  self.stage5, self.stage6, self.stage7, self.stage8]
        for lag in range(8, -1, -1):
            k = t - lag

            @pl.when(jnp.logical_and(k >= 0, k < self.chunks))
            def _(k=k, lag=lag):
                stages[lag](k)

    @property
    def steps(self):
        return self.chunks + 8

    def drain(self):
        counts = [512, 256, 128, 2 * self.piece * (self.place.depth - 1)]
        counts = counts + counts[::-1]
        for i, count in enumerate(counts):
            wait_bytes(self.g.at[pl.ds(0, count * self.chunks), :], self.sent.at[i])


def reduce_kernel(bands, g1_ref, g2_ref, g3_ref, o1_ref, o2_ref, o3_ref, *scratch):
    place = Place(bands)
    hidden = g2_ref.shape[1]
    blocks = hidden // LANES
    chunks = blocks + 2
    red = Reduce(place, chunks, scratch)
    greet_reduce(place)

    for b in range(blocks):
        red.g[pl.ds(b * CHUNK, CHUNK), :] = g2_ref[:, pl.ds(b * LANES, LANES)]
        red.g[pl.ds((blocks + 1) * CHUNK + b * LANES, LANES), :] = g1_ref[:, pl.ds(b * LANES, LANES)]
    red.g[pl.ds(blocks * CHUNK, CHUNK), :] = g3_ref[...]

    @pl.loop(0, red.steps)
    def _(t):
        red.step(t)

    for b in range(blocks):
        o2_ref[:, pl.ds(b * LANES, LANES)] = red.o[pl.ds(b * CHUNK, CHUNK), :]
        o1_ref[:, pl.ds(b * LANES, LANES)] = red.o[pl.ds((blocks + 1) * CHUNK + b * LANES, LANES), :]
    o3_ref[...] = red.o[pl.ds(blocks * CHUNK, CHUNK), :]
    red.drain()


def fits_reduce(bands, pairs, features, hidden):
    return pairs == 2 and bands % 8 == 0 and bands <= 32 and features == LANES and hidden == CHUNK


def reduce_totals(totals):
    bands, pairs = lax.axis_size("lat"), lax.axis_size("dp")
    features, hidden = totals[0].shape
    if not fits_reduce(bands, pairs, features, hidden):
        return lax.psum(tuple(totals), ("lat", "dp"))
    vmem = pl.BlockSpec(memory_space=pltpu.VMEM)
    return pl.pallas_call(
        functools.partial(reduce_kernel, bands),
        in_specs=[vmem] * 3,
        out_specs=[vmem] * 3,
        out_shape=[jax.ShapeDtypeStruct(t.shape, t.dtype) for t in totals],
        scratch_shapes=Reduce.scratch(hidden // LANES + 2, bands // 4),
        compiler_params=pltpu.CompilerParams(
            collective_id=3, has_side_effects=True, vmem_limit_bytes=56 * 2**20
        ),
    )(*totals)


def split_dot(high_low, value, turned=False):
    hi = value.astype(jnp.bfloat16)
    lo = (value - hi.astype(jnp.float32)).astype(jnp.bfloat16)
    table_hi, table_lo = high_low
    mul = t_mul if turned else lambda a, b: jnp.dot(a, b, preferred_element_type=jnp.float32)
    return mul(table_hi, hi) + (mul(table_hi, lo) + mul(table_lo, hi))


def halves(value):
    hi = value.astype(jnp.bfloat16)
    return hi, (value - hi.astype(jnp.float32)).astype(jnp.bfloat16)


class Sizes:
    def __init__(self, bands, lat_rows, lon, features, hidden):
        self.bands, self.lat_rows, self.lon = bands, lat_rows, lon
        self.features, self.hidden = features, hidden
        self.lats = bands * lat_rows
        self.waves = MW // bands
        self.pairs = 2 * self.waves
        self.block = self.pairs * lat_rows
        self.rows = lat_rows * lon
        self.all_pairs = 2 * MW


class Exchange:
    @staticmethod
    def sems(size):
        return [pltpu.SemaphoreType.DMA, pltpu.SemaphoreType.DMA((size.bands,))]

    def __init__(self, size, out, got, ssem, rsem):
        self.size, self.out, self.got, self.ssem, self.rsem = size, out, got, ssem, rsem
        self.me = lax.axis_index("lat")

    def part(self, ref, band, first, count):
        return ref.at[pl.ds(pl.multiple_of(band * self.size.block + first, 8), count), :]

    def start(self, first=0, count=None):
        count = self.size.block if count is None else count

        @pl.loop(1, self.size.bands)
        def _(step):
            to = lax.rem(self.me + step, self.size.bands)
            send(self.part(self.out, to, first, count), self.part(self.got, self.me, first, count),
                 self.ssem, self.rsem.at[step], {"lat": to})

        self.part(self.got, self.me, first, count)[...] = self.part(self.out, self.me, first, count)[...]

    def wait(self):
        @pl.loop(1, self.size.bands)
        def _(step):
            wait_bytes(self.part(self.got, 0, 0, self.size.block), self.rsem.at[step])

    def drain(self):
        wait_bytes(self.out.at[pl.ds(0, (self.size.bands - 1) * self.size.block), :], self.ssem)


def greet_lat(size, also=0):
    me = lax.axis_index("lat")

    @pl.loop(1, size.bands)
    def _(step):
        signal_to({"lat": lax.rem(me + step, size.bands)})


def greeted(count):
    pl.semaphore_wait(pltpu.get_barrier_semaphore(), count)


def build_operator(size, table_ref, quad_ref, op_hi, op_lo):
    quad = quad_ref[...]
    for m in range(size.waves):
        table = table_ref[m]
        base = split_dot(halves(table), table, turned=True)
        hi, lo = halves(base * quad)
        op_hi[m] = hi
        op_lo[m] = lo


def legendre(size, op_hi, op_lo, got, out, turned):
    for m in range(size.waves):
        value = jnp.concatenate(
            [got[pl.ds(2 * m + p, size.lats, stride=size.pairs), :] for p in (0, 1)], axis=1)
        back = split_dot((op_hi[m], op_lo[m]), value, turned)
        for p in (0, 1):
            for d in range(size.bands):
                out[pl.ds(d * size.block + (2 * m + p) * size.lat_rows, size.lat_rows), :] = (
                    back[d * size.lat_rows:(d + 1) * size.lat_rows, p * LANES:(p + 1) * LANES])


def analyse(size, high_low, first, second, lat, out):
    wav = split_dot(high_low, jnp.concatenate([first, second], axis=1))
    for u in (0, 1):
        for d in range(size.bands):
            out[pl.ds(pl.multiple_of(d * size.block + (lat + u) * size.pairs, 8), size.pairs), :] = (
                wav[d * size.pairs:(d + 1) * size.pairs, u * LANES:(u + 1) * LANES])


def synthesise(size, high_low, got, put):
    for lat in range(0, size.lat_rows, 2):
        value = jnp.concatenate(
            [got[pl.ds(lat + u, size.all_pairs, stride=size.lat_rows), :] for u in (0, 1)], axis=1)
        out = split_dot(high_low, value)
        for u in (0, 1):
            put(lat + u, out[:, u * LANES:(u + 1) * LANES])


def forward_tile(size, row, x, w1, w2, w3, keep):
    h1t, s1_ref, h2t, s2_ref, xt = keep
    rows = x.astype(jnp.bfloat16)
    span = pl.ds(row, size.lon)
    if xt is not None:
        xt[:, span] = rows.T
    h1, s1 = silu_pair(jnp.dot(rows, w1[...], preferred_element_type=jnp.float32))
    h1 = h1.astype(jnp.bfloat16)
    s1_ref[span, :] = s1.astype(jnp.bfloat16)
    h1t[:, span] = h1.T
    h2, s2 = silu_pair(jnp.dot(h1, w2[...], preferred_element_type=jnp.float32))
    h2 = h2.astype(jnp.bfloat16)
    s2_ref[span, :] = s2.astype(jnp.bfloat16)
    h2t[:, span] = h2.T
    return x + tend_weight * jnp.dot(h2, w3[...], preferred_element_type=jnp.float32)


def table_copy(size, table_hbm, table_ref, sem):
    waves = size.waves
    return pltpu.make_async_copy(table_hbm.at[pl.ds(lax.axis_index("lat") * waves, waves)], table_ref, sem)


def first_kernel(size, x_ref, c_ref, w1, w2, w3, table_hbm, quad, ana_hi, ana_lo, syt_hi, syt_lo, syn_hi, syn_lo,
                 q_ref, backc_ref, h1t_hbm, s1_hbm, h2t_hbm, s2_hbm,
                 table, op_hi, op_lo, h1t, s1, h2t, s2, outc, gotc, outm, gotm, backm, got2m,
                 tsem, ksems, *sems):
    xc = Exchange(size, outc, gotc, *sems[0:2])
    xm = Exchange(size, outm, gotm, *sems[2:4])
    x2 = Exchange(size, backm, got2m, *sems[4:6])
    greet_lat(size)
    table_in = table_copy(size, table_hbm, table, tsem)
    table_in.start()

    @pl.loop(0, size.lat_rows // 2)
    def _(i):
        analyse(size, (syt_hi[...], syt_lo[...]), c_ref[2 * i], c_ref[2 * i + 1], 2 * i, outc)

    greeted(size.bands - 1)
    xc.start()
    table_in.wait()
    build_operator(size, table, quad, op_hi, op_lo)
    keeps = ((h1t, h1t_hbm, 1), (s1, s1_hbm, 0), (h2t, h2t_hbm, 1), (s2, s2_hbm, 0))

    def keep_copies(i):
        span = pl.ds(pl.multiple_of(i * 2 * size.lon, 2 * size.lon), 2 * size.lon)
        for k, (src, dst, axis) in enumerate(keeps):
            where = (slice(None), span) if axis else (span, slice(None))
            pltpu.make_async_copy(src.at[where], dst.at[where], ksems.at[k]).start()

    @pl.loop(0, size.lat_rows // 2)
    def _(i):
        moved = [
            forward_tile(size, pl.multiple_of((2 * i + u) * size.lon, size.lon), x_ref[2 * i + u],
                         w1, w2, w3, (h1t, s1, h2t, s2, None))
            for u in (0, 1)
        ]
        analyse(size, (ana_hi[...], ana_lo[...]), moved[0], moved[1], 2 * i, outm)
        xm.start(pl.multiple_of(2 * i * size.pairs, 2 * size.pairs), 2 * size.pairs)
        keep_copies(i)

    xc.wait()
    legendre(size, op_hi, op_lo, gotc, backc_ref, True)
    xm.wait()
    legendre(size, op_hi, op_lo, gotm, backm, False)
    x2.start()
    x2.wait()

    def put(lat, value):
        q_ref[lat] = value

    synthesise(size, (syn_hi[...], syn_lo[...]), got2m, put)
    for x in (xc, xm, x2):
        x.drain()
    for k, (src, dst, _) in enumerate(keeps):
        pltpu.make_async_copy(src, dst, ksems.at[k]).wait()


def weight_gradients(size, h1t, h2t, xt, gt, ga1, ga2, put):
    blocks = size.hidden // LANES
    dot = lambda a, b: jnp.dot(a, b, preferred_element_type=jnp.float32)
    half = size.hidden // 2
    for top in (0, half):
        put(blocks * CHUNK + top, dot(h2t[pl.ds(top, half), :], gt[...]))

    @pl.loop(0, blocks // 2)
    def _(i):
        columns = pl.ds(pl.multiple_of(i * 2 * LANES, 2 * LANES), 2 * LANES)
        for top in (0, half):
            part = dot(h1t[pl.ds(top, half), :], ga2[:, columns])
            for u in (0, 1):
                put(pl.multiple_of((2 * i + u) * CHUNK + top, half), part[:, u * LANES:(u + 1) * LANES])
        part = dot(xt[...], ga1[:, columns])
        for u in (0, 1):
            put(pl.multiple_of((blocks + 1) * CHUNK + (2 * i + u) * LANES, LANES),
                part[:, u * LANES:(u + 1) * LANES])


def middle_kernel(size, q_ref, backc_ref, w1, w2, w3, table_hbm, quad,
                  ana_hi, ana_lo, syt_hi, syt_lo, ant_hi, ant_lo,
                  p_ref, backm_ref, g_hbm,
                  table, op_hi, op_lo, h1t, s1, h2t, s2, xt, pulled, gt, ga1, ga2, g,
                  got2c, outm, gotm, outg, gotg, backg, got2g, tsem, gsem, *sems):
    x2c = Exchange(size, backc_ref, got2c, *sems[0:2])
    xm = Exchange(size, outm, gotm, *sems[2:4])
    xg = Exchange(size, outg, gotg, *sems[4:6])
    x2g = Exchange(size, backg, got2g, *sems[6:8])
    greet_lat(size)
    table_in = table_copy(size, table_hbm, table, tsem)
    table_in.start()
    greeted(size.bands - 1)
    x2c.start()
    table_in.wait()
    build_operator(size, table, quad, op_hi, op_lo)

    @pl.loop(0, size.lat_rows // 2)
    def _(i):
        moved = [
            forward_tile(size, pl.multiple_of((2 * i + u) * size.lon, size.lon), q_ref[2 * i + u],
                         w1, w2, w3, (h1t, s1, h2t, s2, xt))
            for u in (0, 1)
        ]
        analyse(size, (ana_hi[...], ana_lo[...]), moved[0], moved[1], 2 * i, outm)

    x2c.wait()

    def put(lat, value):
        pulled[lat] = value

    synthesise(size, (ant_hi[...], ant_lo[...]), got2c, put)
    xm.start()

    @pl.loop(0, size.lat_rows // 2)
    def _(i):
        span = pl.ds(pl.multiple_of(2 * i * size.lon, 2 * size.lon), 2 * size.lon)
        p = jnp.concatenate([pulled[2 * i], pulled[2 * i + 1]], axis=0)
        g_t = (tend_weight * p).astype(jnp.bfloat16)
        gt[span, :] = g_t
        g_a2 = (mul_t(g_t, w3[...]) * s2[span, :].astype(jnp.float32)).astype(jnp.bfloat16)
        ga2[span, :] = g_a2
        g_a1 = (mul_t(g_a2, w2[...]) * s1[span, :].astype(jnp.float32)).astype(jnp.bfloat16)
        ga1[span, :] = g_a1
        grad = p + mul_t(g_a1, w1[...])
        analyse(size, (syt_hi[...], syt_lo[...]), grad[:size.lon], grad[size.lon:], 2 * i, outg)
        xg.start(pl.multiple_of(2 * i * size.pairs, 2 * size.pairs), 2 * size.pairs)

    def keep(row, value):
        g[pl.ds(row, value.shape[0]), :] = value

    weight_gradients(size, h1t, h2t, xt, gt, ga1, ga2, keep)
    xm.wait()
    legendre(size, op_hi, op_lo, gotm, backm_ref, False)
    g_out = pltpu.make_async_copy(g, g_hbm, gsem)
    g_out.start()
    xg.wait()
    legendre(size, op_hi, op_lo, gotg, backg, True)
    x2g.start()
    x2g.wait()

    def put_pulled(lat, value):
        p_ref[lat] = value

    synthesise(size, (ant_hi[...], ant_lo[...]), got2g, put_pulled)
    for x in (x2c, xm, xg, x2g):
        x.drain()
    g_out.wait()


def last_kernel(size, p_ref, x_ref, backm_ref, w2, w3, syn_hi, syn_lo, g_hbm, h1t_hbm, s1_hbm, h2t_hbm, s2_hbm,
                final_ref, o_ref, h1t, s1, h2t, s2, xt, gt, ga1, ga2, got2m, lsems, ssem, rsem, *scratch):
    place = Place(size.bands)
    chunks = size.hidden // LANES + 2
    red = Reduce(place, chunks, (scratch[0], o_ref, *scratch[1:]))
    g = red.g
    x2m = Exchange(size, backm_ref, got2m, ssem, rsem)
    greet_lat(size)
    signal_to(place.across_core)
    loads = [pltpu.make_async_copy(src, dst, lsems.at[k]) for k, (src, dst) in enumerate(
        ((s2_hbm, s2), (h2t_hbm, h2t), (h1t_hbm, h1t), (g_hbm, g), (s1_hbm, s1)))]
    for load in loads:
        load.start()
    greeted(size.bands)
    x2m.start()
    loads[0].wait()

    tiles = size.lat_rows // 2

    def span_of(i):
        return pl.ds(pl.multiple_of(2 * i * size.lon, 2 * size.lon), 2 * size.lon)

    @pl.loop(0, tiles)
    def _(i):
        span = span_of(i)
        xt[:, span] = jnp.concatenate([x_ref[2 * i], x_ref[2 * i + 1]], axis=0).astype(jnp.bfloat16).T
        g_t = (tend_weight * jnp.concatenate([p_ref[2 * i], p_ref[2 * i + 1]], axis=0)).astype(jnp.bfloat16)
        gt[span, :] = g_t
        ga2[span, :] = (mul_t(g_t, w3[...]) * s2[span, :].astype(jnp.float32)).astype(jnp.bfloat16)

    for load in loads[1:]:
        load.wait()

    @pl.loop(0, tiles)
    def _(i):
        span = span_of(i)
        ga1[span, :] = (mul_t(ga2[span, :], w2[...]) * s1[span, :].astype(jnp.float32)).astype(jnp.bfloat16)

    def put(row, value):
        g[pl.ds(row, value.shape[0]), :] += value

    weight_gradients(size, h1t, h2t, xt, gt, ga1, ga2, put)

    @pl.loop(0, red.steps)
    def _(t):
        red.step(t)

    x2m.wait()

    def put_final(lat, value):
        final_ref[lat] = value

    synthesise(size, (syn_hi[...], syn_lo[...]), got2m, put_final)
    x2m.drain()
    red.drain()


def fused_body(size, state, cotangent, w1, w2, w3):
    analysis, synthesis = grid_tables(size.lon, MW)
    table, quad = legendre_tables(size.lats, MW)
    pair = lambda t: [jnp.asarray(part) for part in np_halves(t)]
    ana_t, syn_t = pair(analysis.T), pair(synthesis.T)
    ana, syn = pair(analysis), pair(synthesis)
    table, quad = jnp.asarray(table), jnp.asarray(quad)[None, :]
    vmem = pl.BlockSpec(memory_space=pltpu.VMEM)
    hbm = pl.BlockSpec(memory_space=pl.ANY)
    f32, bf16 = jnp.float32, jnp.bfloat16
    field = jax.ShapeDtypeStruct(state.shape[1:], f32)
    blocks = jax.ShapeDtypeStruct((size.bands * size.block, LANES), f32)
    wide = jax.ShapeDtypeStruct((size.rows, size.hidden), bf16)
    tall = jax.ShapeDtypeStruct((size.hidden, size.rows), bf16)
    grads = jax.ShapeDtypeStruct(((size.hidden // LANES + 2) * CHUNK, LANES), f32)
    buf = lambda shape: pltpu.VMEM(shape.shape, shape.dtype)
    dma = pltpu.SemaphoreType.DMA
    operator = [pltpu.VMEM((size.waves, MW, size.lats), f32)] + [
        pltpu.VMEM((size.waves, size.lats, size.lats), bf16)] * 2
    narrow = pltpu.VMEM((size.rows, LANES), bf16)
    x_t = pltpu.VMEM((LANES, size.rows), bf16)
    work = size.rows * size.hidden * (size.hidden + 2 * size.features)
    call = lambda kernel, ident, flops, ins, outs, shapes, scratch: pl.pallas_call(
        functools.partial(kernel, size), in_specs=ins, out_specs=outs, out_shape=shapes, scratch_shapes=scratch,
        cost_estimate=pl.CostEstimate(flops=flops, bytes_accessed=2**24, transcendentals=0),
        compiler_params=pltpu.CompilerParams(
            collective_id=ident, has_side_effects=True, vmem_limit_bytes=60 * 2**20))
    x0 = state[0]
    q1, back_c, *saved = call(
        first_kernel, 1, 2 * work, [vmem] * 5 + [hbm] + [vmem] * 7, [vmem] * 2 + [hbm] * 4,
        [field, blocks, tall, wide, tall, wide],
        operator + [buf(tall), buf(wide), buf(tall), buf(wide)] + [buf(blocks)] * 6
        + [dma, dma((4,))] + Exchange.sems(size) * 3,
    )(x0, cotangent[0], w1, w2, w3, table, quad, *ana_t, *syn_t, *syn)
    pulled0, back_m, sums = call(
        middle_kernel, 2, 6 * work, [vmem] * 5 + [hbm] + [vmem] * 7, [vmem, vmem, hbm],
        [field, blocks, grads],
        operator + [buf(tall), buf(wide), buf(tall), buf(wide), x_t, buf(field), narrow, buf(wide), buf(wide),
                    buf(grads)]
        + [buf(blocks)] * 7 + [dma, dma] + Exchange.sems(size) * 4,
    )(q1, back_c, w1, w2, w3, table, quad, *ana_t, *syn_t, *ana)
    reduce_scratch = Reduce.scratch(size.hidden // LANES + 2, size.bands // 4)
    final, totals = call(
        last_kernel, 3, 4 * work, [vmem] * 7 + [hbm] * 5, [vmem, vmem], [field, grads],
        [buf(tall), buf(wide), buf(tall), buf(wide), x_t, narrow, buf(wide), buf(wide), buf(blocks), dma((5,))]
        + Exchange.sems(size) + reduce_scratch[:1] + reduce_scratch[2:],
    )(pulled0, x0, back_m, w2, w3, *syn, sums, *saved)
    lanes = size.hidden // LANES
    middle, last, first = totals[:lanes * CHUNK], totals[lanes * CHUNK:(lanes + 1) * CHUNK], totals[(lanes + 1) * CHUNK:]
    unblock = lambda t, rows: t.reshape(lanes, rows, LANES).transpose(1, 0, 2).reshape(rows, size.hidden)
    return final[None], unblock(first, size.features), unblock(middle, size.hidden), last


def np_halves(table):
    hi = table.astype(jnp.bfloat16)
    return hi, (table - hi.astype(np.float32)).astype(jnp.bfloat16)


def fits_fused(size, sample):
    return (sample == 1 and size.lat_rows == 8 and size.pairs == 8 and size.lon % 256 == 0
            and size.lats % LANES == 0 and size.bands % 8 == 0)


def body(state, cotangent, w1, w2, w3):
    sample, lat_rows, lon_count, features = state.shape
    bands = lax.axis_size("lat")
    size = Sizes(bands, lat_rows, lon_count, features, w1.shape[1])
    if fits_fused(size, sample) and fits_reduce(bands, lax.axis_size("dp"), features, w1.shape[1]):
        return fused_body(size, state, cotangent, w1, w2, w3)
    lat_count = lat_rows * bands
    waves = MW // bands
    analysis, synthesis = grid_tables(lon_count, MW)
    table, quad = legendre_tables(lat_count, MW)
    mine = lax.dynamic_slice_in_dim(jnp.asarray(table), lax.axis_index("lat") * waves, waves, axis=0)
    base = jnp.einsum("mki,mkj->mij", mine, mine, precision=lax.Precision.HIGHEST)
    quad = jnp.asarray(quad)
    forward_op = base * quad[None, None, :]
    backward_op = base * quad[None, :, None]

    def spectral(parts):
        sent = []
        for field, first, _, _ in parts:
            wav = jnp.einsum("bjxf,xq->bqjf", field, first, precision=high)
            sent.append(wav.reshape(sample, bands, waves * 2, lat_rows, features))
        sent = jnp.concatenate(sent, axis=0).transpose(1, 0, 2, 3, 4)
        got = lax.all_to_all(sent, "lat", split_axis=0, concat_axis=0, tiled=True)
        got = got.reshape(bands, len(parts), sample, waves, 2, lat_rows, features)
        ops = jnp.stack([p[2] for p in parts]).reshape(len(parts), waves, bands, lat_rows, lat_count)
        got = got.transpose(1, 3, 0, 5, 2, 4, 6).reshape(len(parts), waves, lat_count, -1)
        ops = ops.reshape(len(parts), waves, lat_count, lat_count)
        back = jnp.einsum("smij,smjv->smiv", ops, got, precision=high)
        back = back.reshape(len(parts), waves, bands, lat_rows, sample, 2, features)
        back = back.transpose(2, 0, 4, 1, 5, 3, 6)
        back = lax.all_to_all(back, "lat", split_axis=0, concat_axis=0, tiled=True)
        out = []
        for index, (_, _, _, last) in enumerate(parts):
            piece = back[:, index].transpose(1, 0, 2, 3, 4, 5)
            piece = piece.reshape(sample, MW * 2, lat_rows, features)
            out.append(jnp.einsum("bqjf,xq->bjxf", piece, last, precision=high))
        return out

    flat = lambda field: field.reshape(sample * lat_rows * lon_count, features)
    x0 = flat(state)
    moved0, *saved0 = forward_rows(x0, w1, w2, w3)
    (pulled1,) = spectral([(cotangent, synthesis, backward_op, analysis)])
    (q1,) = spectral([(moved0.reshape(state.shape), analysis, forward_op, synthesis)])
    x1 = flat(q1)
    moved1, *saved1 = forward_rows(x1, w1, w2, w3)
    *totals, grad = backward_rows(flat(pulled1), x1, saved1, w1, w2, w3, None, True)
    (final,) = spectral([(moved1.reshape(state.shape), analysis, forward_op, synthesis)])
    (pulled0,) = spectral([(grad.reshape(state.shape), synthesis, backward_op, analysis)])
    totals = backward_rows(flat(pulled0), x0, saved0, w1, w2, w3, totals, False)
    totals = reduce_totals(totals)
    return (final, *totals)


def solution(mesh):
    field = P("dp", "lat", None, None)
    return jax.shard_map(
        body, mesh=mesh, in_specs=(field, field, P(), P(), P()),
        out_specs=(field, P(), P(), P()), check_vma=False,
    )
```

```python
import functools
import math

import jax
import jax.numpy as jnp
import numpy as np
from jax import lax
from jax.experimental import pallas as pl
from jax.experimental.pallas import tpu as pltpu
from jax.sharding import PartitionSpec as P

MW = 64
STEPS = 2

high = lax.Precision.HIGH
tend_weight = 0.5


def grid_tables(lon_count, wave_count):
    lon_index = np.arange(lon_count)
    wave_index = np.arange(wave_count)
    angle = 2.0 * math.pi * (lon_index[:, None] * wave_index[None, :] % lon_count) / lon_count
    pair = np.stack([np.cos(angle), -np.sin(angle)], axis=2)
    factor = np.where(wave_index == 0, 1.0, 2.0)
    analysis = (pair / lon_count).reshape(lon_count, -1).astype(np.float32)
    synthesis = (pair * factor[None, :, None]).reshape(lon_count, -1).astype(np.float32)
    return analysis, synthesis


def legendre_tables(lat_count, wave_count):
    latitude = -0.5 * math.pi + (np.arange(lat_count) + 0.5) * math.pi / lat_count
    mu, cosine = np.sin(latitude), np.cos(latitude)
    quad_weight = cosine * math.pi / lat_count
    order = np.arange(wave_count, dtype=np.float64)
    steps = np.concatenate([[0.0], 0.5 * np.log((2 * order[1:] + 1) / (2 * order[1:]))])
    diagonal = np.exp(
        0.5 * math.log(0.5) + np.cumsum(steps)[:, None] + order[:, None] * np.log(cosine)[None, :]
    )
    rows = [diagonal]
    previous, current, ratio_prev = np.zeros_like(diagonal), diagonal, np.ones_like(order)
    for offset in range(1, wave_count):
        n = order + offset
        ratio = np.sqrt((4 * n * n - 1) / (n * n - order * order))
        following = ratio[:, None] * (mu[None, :] * current - previous / ratio_prev[:, None])
        previous, current, ratio_prev = current, following, ratio
        rows.append(following)
    table = np.stack(rows, axis=1)
    degree = order[:, None] + np.arange(wave_count)[None, :]
    kept = degree <= wave_count - 1
    damping = np.where(kept, 1.0 / (1.0 + degree * (degree + 1) / (wave_count * (wave_count - 1.0))), 0.0)
    table = np.where(kept[:, :, None], table, 0.0) * np.sqrt(damping)[:, :, None]
    return table.astype(np.float32), quad_weight.astype(np.float32)


def silu_pair(value):
    gate = 0.5 * jnp.tanh(0.5 * value) + 0.5
    hidden = value * gate
    return hidden, gate + hidden - hidden * gate


def forward_kernel(x_ref, w1_ref, w2_ref, w3_ref, moved_ref, h1_ref, s1_ref, h2_ref, s2_ref):
    field = x_ref[...]
    rows = field.astype(jnp.bfloat16)
    h1, s1 = silu_pair(jnp.dot(rows, w1_ref[...], preferred_element_type=jnp.float32))
    h1 = h1.astype(jnp.bfloat16)
    h1_ref[...] = h1
    s1_ref[...] = s1.astype(jnp.bfloat16)
    h2, s2 = silu_pair(jnp.dot(h1, w2_ref[...], preferred_element_type=jnp.float32))
    h2 = h2.astype(jnp.bfloat16)
    h2_ref[...] = h2
    s2_ref[...] = s2.astype(jnp.bfloat16)
    tend = jnp.dot(h2, w3_ref[...], preferred_element_type=jnp.float32)
    moved_ref[...] = field + tend_weight * tend


def forward_rows(x, w1, w2, w3):
    count, features = x.shape
    hidden = w1.shape[1]
    tile = math.gcd(count, 256)
    row = lambda width: pl.BlockSpec((tile, width), lambda i: (i, 0))
    whole = lambda w: pl.BlockSpec(w.shape, lambda i: (0, 0))
    wide = jax.ShapeDtypeStruct((count, hidden), jnp.bfloat16)
    return pl.pallas_call(
        forward_kernel,
        grid=(count // tile,),
        in_specs=[row(features), whole(w1), whole(w2), whole(w3)],
        out_specs=[row(features)] + [row(hidden)] * 4,
        out_shape=[jax.ShapeDtypeStruct(x.shape, jnp.float32)] + [wide] * 4,
        cost_estimate=pl.CostEstimate(
            flops=2 * count * (2 * features * hidden + hidden * hidden),
            bytes_accessed=count * hidden * 8, transcendentals=2 * count * hidden,
        ),
        compiler_params=pltpu.CompilerParams(dimension_semantics=("arbitrary",)),
    )(x, w1, w2, w3)


def mul_t(a, b):
    return lax.dot_general(a, b, (((1,), (1,)), ((), ())), preferred_element_type=jnp.float32)


def t_mul(a, b):
    return lax.dot_general(a, b, (((0,), (0,)), ((), ())), preferred_element_type=jnp.float32)


def backward_kernel(first_call, need_rows, *refs):
    p_ref, x_ref, h1_ref, s1_ref, h2_ref, s2_ref, w1_ref, w2_ref, w3_ref = refs[:9]
    refs = refs[9:]
    if not first_call:
        c1_ref, c2_ref, c3_ref = refs[:3]
        refs = refs[3:]
    g1_ref, g2_ref, g3_ref = refs[:3]

    @pl.when(pl.program_id(0) == 0)
    def _():
        if first_call:
            g1_ref[...] = jnp.zeros_like(g1_ref)
            g2_ref[...] = jnp.zeros_like(g2_ref)
            g3_ref[...] = jnp.zeros_like(g3_ref)
        else:
            g1_ref[...] = c1_ref[...]
            g2_ref[...] = c2_ref[...]
            g3_ref[...] = c3_ref[...]

    pulled = p_ref[...]
    gt = (tend_weight * pulled).astype(jnp.bfloat16)
    g3_ref[...] += t_mul(h2_ref[...], gt)
    ga2 = (mul_t(gt, w3_ref[...]) * s2_ref[...].astype(jnp.float32)).astype(jnp.bfloat16)
    g2_ref[...] += t_mul(h1_ref[...], ga2)
    ga1 = (mul_t(ga2, w2_ref[...]) * s1_ref[...].astype(jnp.float32)).astype(jnp.bfloat16)
    g1_ref[...] += t_mul(x_ref[...].astype(jnp.bfloat16), ga1)
    if need_rows:
        refs[3][...] = pulled + mul_t(ga1, w1_ref[...])


def backward_rows(pulled, x, saved, w1, w2, w3, carry, need_rows):
    count, features = x.shape
    hidden = w1.shape[1]
    tile = math.gcd(count, 512)
    row = lambda width: pl.BlockSpec((tile, width), lambda i: (i, 0))
    whole = lambda w: pl.BlockSpec(w.shape, lambda i: (0, 0))
    out_shape = [jax.ShapeDtypeStruct(w.shape, jnp.float32) for w in (w1, w2, w3)]
    out_specs = [whole(w) for w in (w1, w2, w3)]
    carried = [] if carry is None else list(carry)
    if need_rows:
        out_shape.append(jax.ShapeDtypeStruct(x.shape, jnp.float32))
        out_specs.append(row(features))
    return pl.pallas_call(
        functools.partial(backward_kernel, carry is None, need_rows),
        grid=(count // tile,),
        in_specs=[row(features)] * 2 + [row(hidden)] * 4
        + [whole(w) for w in (w1, w2, w3)] + [whole(c) for c in carried],
        out_specs=out_specs,
        out_shape=out_shape,
        cost_estimate=pl.CostEstimate(
            flops=4 * count * (2 * features * hidden + hidden * hidden),
            bytes_accessed=count * hidden * 8, transcendentals=0,
        ),
        compiler_params=pltpu.CompilerParams(dimension_semantics=("arbitrary",)),
    )(pulled, x, *saved, w1, w2, w3, *carried)


MESH_ID = pl.DeviceIdType.MESH
LANES = 128
CHUNK = 1024
SPAN = CHUNK
HALF = SPAN // 2
LAGS = (0, 1, 3, 5, 7, 9, 11, 13, 14)


class Place:
    def __init__(self, bands):
        self.me = lax.axis_index("lat")
        self.core = lax.axis_index("dp")
        self.depth = bands // 4
        self.x = lax.rem(self.me, 2)
        self.y = lax.rem(self.me // 2, 2)
        self.z = self.me // 4
        self.across_core = {"dp": 1 - self.core}
        self.across_x = {"lat": self.me + 1 - 2 * self.x}
        self.across_y = {"lat": self.me + 2 - 4 * self.y}

    def along_z(self, step):
        layer = lax.rem(self.z + step, self.depth)
        return layer, {"lat": layer * 4 + lax.rem(self.me, 4)}


def signal_to(device):
    pl.semaphore_signal(pltpu.get_barrier_semaphore(), inc=1, device_id=device, device_id_type=MESH_ID)


def greet_reduce(place):
    signal_to(place.across_core)
    signal_to(place.across_x)
    signal_to(place.across_y)
    for step in range(1, place.depth):
        signal_to(place.along_z(step)[1])
    pl.semaphore_wait(pltpu.get_barrier_semaphore(), place.depth + 2)


def send(src, dst, ssem, rsem, device):
    pltpu.make_async_remote_copy(
        src_ref=src, dst_ref=dst, send_sem=ssem, recv_sem=rsem, device_id=device, device_id_type=MESH_ID
    ).start()


def wait_bytes(ref, sem):
    pltpu.make_async_copy(ref, ref, sem).wait()


class Reduce:
    SENDS = 8

    @staticmethod
    def scratch(chunks, depth):
        rows = lambda parts: pltpu.VMEM((chunks * SPAN // parts, LANES), jnp.float32)
        sems = lambda *dims: pltpu.SemaphoreType.DMA((chunks,) + dims)
        return [
            rows(1), rows(1), rows(2), rows(4), rows(8),
            pltpu.VMEM((chunks, depth - 1, SPAN // 8 // depth, LANES), jnp.float32),
            sems(), sems(2), sems(2), sems(depth - 1), sems(depth - 1), sems(2), sems(2), sems(),
            pltpu.SemaphoreType.DMA((Reduce.SENDS,)),
        ]

    def __init__(self, place, chunks, refs):
        (self.g, self.o, self.r0, self.r1, self.r2, self.r3,
         self.d0, self.m1, self.m2, self.z3, self.z4, self.m5, self.m6, self.d7, self.sent) = refs
        self.place, self.chunks = place, chunks
        self.piece = SPAN // 16 // place.depth
        p = place
        half = p.core * HALF
        self.first = ((p.across_x, p.x), (p.across_y, p.y))
        self.second = (self.first[1], self.first[0])
        self.quarter = (half, half + HALF // 2)
        self.eighth = tuple(self.quarter[i] + self.first[i][1] * (HALF // 4) for i in (0, 1))
        self.sixteenth = tuple(self.eighth[i] + self.second[i][1] * (HALF // 8) for i in (0, 1))
        self.own = tuple(self.sixteenth[i] + p.z * self.piece for i in (0, 1))

    def rows(self, ref, k, offset, count, span=SPAN):
        return ref.at[pl.ds(pl.multiple_of(k * span + offset, 8), count), :]

    def stage0(self, k):
        other = (1 - self.place.core) * HALF
        send(self.rows(self.g, k, other, HALF), self.rows(self.r0, k, 0, HALF, HALF),
             self.sent.at[0], self.d0.at[k], self.place.across_core)

    def stage1(self, k):
        wait_bytes(self.rows(self.r0, k, 0, HALF, HALF), self.d0.at[k])
        mine = self.rows(self.g, k, self.place.core * HALF, HALF)
        mine[...] += self.rows(self.r0, k, 0, HALF, HALF)[...]
        for i in (0, 1):
            device, bit = self.first[i]
            send(self.rows(self.g, k, self.quarter[i] + (1 - bit) * (HALF // 4), HALF // 4),
                 self.rows(self.r1, k, i * (HALF // 4), HALF // 4, HALF // 2), self.sent.at[1], self.m1.at[k, i], device)

    def stage2(self, k):
        for i in (0, 1):
            got = self.rows(self.r1, k, i * (HALF // 4), HALF // 4, HALF // 2)
            wait_bytes(got, self.m1.at[k, i])
            self.rows(self.g, k, self.eighth[i], HALF // 4)[...] += got[...]
        for i in (0, 1):
            device, bit = self.second[i]
            send(self.rows(self.g, k, self.eighth[i] + (1 - bit) * (HALF // 8), HALF // 8),
                 self.rows(self.r2, k, i * (HALF // 8), HALF // 8, HALF // 4), self.sent.at[2], self.m2.at[k, i], device)

    def stage3(self, k):
        for i in (0, 1):
            got = self.rows(self.r2, k, i * (HALF // 8), HALF // 8, HALF // 4)
            wait_bytes(got, self.m2.at[k, i])
            self.rows(self.g, k, self.sixteenth[i], HALF // 8)[...] += got[...]
        for step in range(1, self.place.depth):
            layer, device = self.place.along_z(step)
            for i in (0, 1):
                send(self.rows(self.g, k, self.sixteenth[i] + layer * self.piece, self.piece),
                     self.r3.at[k, step - 1, pl.ds(i * self.piece, self.piece), :],
                     self.sent.at[3], self.z3.at[k, step - 1], device)

    def stage4(self, k):
        total = [self.rows(self.g, k, self.own[i], self.piece)[...] for i in (0, 1)]
        for step in range(1, self.place.depth):
            wait_bytes(self.r3.at[k, step - 1], self.z3.at[k, step - 1])
            for i in (0, 1):
                total[i] += self.r3[k, step - 1, pl.ds(i * self.piece, self.piece), :]
        for i in (0, 1):
            self.rows(self.o, k, self.own[i], self.piece)[...] = total[i]
        for step in range(1, self.place.depth):
            _, device = self.place.along_z(step)
            for i in (0, 1):
                mine = self.rows(self.o, k, self.own[i], self.piece)
                send(mine, mine, self.sent.at[4], self.z4.at[k, step - 1], device)

    def stage5(self, k):
        for step in range(1, self.place.depth):
            wait_bytes(self.r3.at[k, step - 1], self.z4.at[k, step - 1])
        for i in (0, 1):
            mine = self.rows(self.o, k, self.sixteenth[i], HALF // 8)
            send(mine, mine, self.sent.at[5], self.m5.at[k, i], self.second[i][0])

    def stage6(self, k):
        for i in (0, 1):
            wait_bytes(self.rows(self.r2, k, 0, HALF // 8, HALF // 4), self.m5.at[k, i])
        for i in (0, 1):
            mine = self.rows(self.o, k, self.eighth[i], HALF // 4)
            send(mine, mine, self.sent.at[6], self.m6.at[k, i], self.first[i][0])

    def stage7(self, k):
        for i in (0, 1):
            wait_bytes(self.rows(self.r1, k, 0, HALF // 4, HALF // 2), self.m6.at[k, i])
        mine = self.rows(self.o, k, self.place.core * HALF, HALF)
        send(mine, mine, self.sent.at[7], self.d7.at[k], self.place.across_core)

    def stage8(self, k):
        wait_bytes(self.rows(self.r0, k, 0, HALF, HALF), self.d7.at[k])

    def step(self, t):
        stages = [self.stage0, self.stage1, self.stage2, self.stage3, self.stage4,
                  self.stage5, self.stage6, self.stage7, self.stage8]
        for stage, lag in reversed(list(zip(stages, LAGS))):
            k = t - lag

            @pl.when(jnp.logical_and(k >= 0, k < self.chunks))
            def _(k=k, stage=stage):
                stage(k)

    @property
    def steps(self):
        return self.chunks + LAGS[-1]

    def drain(self):
        counts = [HALF, HALF // 2, HALF // 4, 2 * self.piece * (self.place.depth - 1)]
        counts = counts + counts[::-1]
        for i, count in enumerate(counts):
            wait_bytes(self.g.at[pl.ds(0, count * self.chunks), :], self.sent.at[i])


def reduce_kernel(bands, g1_ref, g2_ref, g3_ref, o1_ref, o2_ref, o3_ref, *scratch):
    place = Place(bands)
    hidden = g2_ref.shape[1]
    blocks = hidden // LANES
    chunks = blocks + 2
    red = Reduce(place, chunks, scratch)
    greet_reduce(place)

    for b in range(blocks):
        red.g[pl.ds(b * CHUNK, CHUNK), :] = g2_ref[:, pl.ds(b * LANES, LANES)]
        red.g[pl.ds((blocks + 1) * CHUNK + b * LANES, LANES), :] = g1_ref[:, pl.ds(b * LANES, LANES)]
    red.g[pl.ds(blocks * CHUNK, CHUNK), :] = g3_ref[...]

    @pl.loop(0, red.steps)
    def _(t):
        red.step(t)

    for b in range(blocks):
        o2_ref[:, pl.ds(b * LANES, LANES)] = red.o[pl.ds(b * CHUNK, CHUNK), :]
        o1_ref[:, pl.ds(b * LANES, LANES)] = red.o[pl.ds((blocks + 1) * CHUNK + b * LANES, LANES), :]
    o3_ref[...] = red.o[pl.ds(blocks * CHUNK, CHUNK), :]
    red.drain()


def fits_reduce(bands, pairs, features, hidden):
    return pairs == 2 and bands % 8 == 0 and bands <= 32 and features == LANES and hidden == CHUNK


def reduce_totals(totals):
    bands, pairs = lax.axis_size("lat"), lax.axis_size("dp")
    features, hidden = totals[0].shape
    if not fits_reduce(bands, pairs, features, hidden):
        return lax.psum(tuple(totals), ("lat", "dp"))
    vmem = pl.BlockSpec(memory_space=pltpu.VMEM)
    return pl.pallas_call(
        functools.partial(reduce_kernel, bands),
        in_specs=[vmem] * 3,
        out_specs=[vmem] * 3,
        out_shape=[jax.ShapeDtypeStruct(t.shape, t.dtype) for t in totals],
        scratch_shapes=Reduce.scratch(hidden // LANES + 2, bands // 4),
        compiler_params=pltpu.CompilerParams(
            collective_id=3, has_side_effects=True, vmem_limit_bytes=56 * 2**20
        ),
    )(*totals)


def split_dot(high_low, value, turned=False):
    hi = value.astype(jnp.bfloat16)
    lo = (value - hi.astype(jnp.float32)).astype(jnp.bfloat16)
    table_hi, table_lo = high_low
    mul = t_mul if turned else lambda a, b: jnp.dot(a, b, preferred_element_type=jnp.float32)
    return mul(table_hi, hi) + (mul(table_hi, lo) + mul(table_lo, hi))


def halves(value):
    hi = value.astype(jnp.bfloat16)
    return hi, (value - hi.astype(jnp.float32)).astype(jnp.bfloat16)


class Sizes:
    def __init__(self, bands, lat_rows, lon, features, hidden):
        self.bands, self.lat_rows, self.lon = bands, lat_rows, lon
        self.features, self.hidden = features, hidden
        self.lats = bands * lat_rows
        self.waves = MW // bands
        self.pairs = 2 * self.waves
        self.block = self.pairs * lat_rows
        self.rows = lat_rows * lon
        self.all_pairs = 2 * MW


class Exchange:
    @staticmethod
    def sems(size):
        return [pltpu.SemaphoreType.DMA, pltpu.SemaphoreType.DMA((size.bands,))]

    def __init__(self, size, out, got, ssem, rsem):
        self.size, self.out, self.got, self.ssem, self.rsem = size, out, got, ssem, rsem
        self.me = lax.axis_index("lat")

    def part(self, ref, band, first, count):
        return ref.at[pl.ds(pl.multiple_of(band * self.size.block + first, 8), count), :]

    def start(self, first=0, count=None):
        count = self.size.block if count is None else count

        @pl.loop(1, self.size.bands)
        def _(step):
            to = lax.rem(self.me + step, self.size.bands)
            send(self.part(self.out, to, first, count), self.part(self.got, self.me, first, count),
                 self.ssem, self.rsem.at[step], {"lat": to})

        self.part(self.got, self.me, first, count)[...] = self.part(self.out, self.me, first, count)[...]

    def wait(self):
        @pl.loop(1, self.size.bands)
        def _(step):
            wait_bytes(self.part(self.got, 0, 0, self.size.block), self.rsem.at[step])

    def drain(self):
        wait_bytes(self.out.at[pl.ds(0, (self.size.bands - 1) * self.size.block), :], self.ssem)


def greet_lat(size, also=0):
    me = lax.axis_index("lat")

    @pl.loop(1, size.bands)
    def _(step):
        signal_to({"lat": lax.rem(me + step, size.bands)})


def greeted(count):
    pl.semaphore_wait(pltpu.get_barrier_semaphore(), count)


def build_operator(size, table_ref, quad_ref, op_hi, op_lo):
    quad = quad_ref[...]
    for m in range(size.waves):
        table = table_ref[m]
        base = split_dot(halves(table), table, turned=True)
        hi, lo = halves(base * quad)
        op_hi[m] = hi
        op_lo[m] = lo


def legendre(size, op_hi, op_lo, got, out, turned):
    for m in range(size.waves):
        value = jnp.concatenate(
            [got[pl.ds(2 * m + p, size.lats, stride=size.pairs), :] for p in (0, 1)], axis=1)
        back = split_dot((op_hi[m], op_lo[m]), value, turned)
        for p in (0, 1):
            for d in range(size.bands):
                out[pl.ds(d * size.block + (2 * m + p) * size.lat_rows, size.lat_rows), :] = (
                    back[d * size.lat_rows:(d + 1) * size.lat_rows, p * LANES:(p + 1) * LANES])


def analyse(size, high_low, first, second, lat, out):
    wav = split_dot(high_low, jnp.concatenate([first, second], axis=1))
    for u in (0, 1):
        for d in range(size.bands):
            out[pl.ds(pl.multiple_of(d * size.block + (lat + u) * size.pairs, 8), size.pairs), :] = (
                wav[d * size.pairs:(d + 1) * size.pairs, u * LANES:(u + 1) * LANES])


def synthesise(size, high_low, got, put):
    for lat in range(0, size.lat_rows, 2):
        value = jnp.concatenate(
            [got[pl.ds(lat + u, size.all_pairs, stride=size.lat_rows), :] for u in (0, 1)], axis=1)
        out = split_dot(high_low, value)
        for u in (0, 1):
            put(lat + u, out[:, u * LANES:(u + 1) * LANES])


def forward_tile(size, row, x, w1, w2, w3, keep):
    h1t, s1_ref, h2t, s2_ref, xt = keep
    rows = x.astype(jnp.bfloat16)
    span = pl.ds(row, size.lon)
    if xt is not None:
        xt[:, span] = rows.T
    h1, s1 = silu_pair(jnp.dot(rows, w1[...], preferred_element_type=jnp.float32))
    h1 = h1.astype(jnp.bfloat16)
    s1_ref[span, :] = s1.astype(jnp.bfloat16)
    h1t[:, span] = h1.T
    h2, s2 = silu_pair(jnp.dot(h1, w2[...], preferred_element_type=jnp.float32))
    h2 = h2.astype(jnp.bfloat16)
    s2_ref[span, :] = s2.astype(jnp.bfloat16)
    h2t[:, span] = h2.T
    return x + tend_weight * jnp.dot(h2, w3[...], preferred_element_type=jnp.float32)


def table_copy(size, table_hbm, table_ref, sem):
    waves = size.waves
    return pltpu.make_async_copy(table_hbm.at[pl.ds(lax.axis_index("lat") * waves, waves)], table_ref, sem)


def first_kernel(size, x_ref, c_ref, w1, w2, w3, table_hbm, quad, ana_hi, ana_lo, syt_hi, syt_lo, syn_hi, syn_lo,
                 q_ref, backc_ref, h1t_hbm, s1_hbm, h2t_hbm, s2_hbm,
                 table, op_hi, op_lo, h1t, s1, h2t, s2, outc, gotc, outm, gotm, backm, got2m,
                 tsem, ksems, *sems):
    xc = Exchange(size, outc, gotc, *sems[0:2])
    xm = Exchange(size, outm, gotm, *sems[2:4])
    x2 = Exchange(size, backm, got2m, *sems[4:6])
    greet_lat(size)
    table_in = table_copy(size, table_hbm, table, tsem)
    table_in.start()

    @pl.loop(0, size.lat_rows // 2)
    def _(i):
        analyse(size, (syt_hi[...], syt_lo[...]), c_ref[2 * i], c_ref[2 * i + 1], 2 * i, outc)

    greeted(size.bands - 1)
    xc.start()
    table_in.wait()
    build_operator(size, table, quad, op_hi, op_lo)
    keeps = ((h1t, h1t_hbm, 1), (s1, s1_hbm, 0), (h2t, h2t_hbm, 1), (s2, s2_hbm, 0))

    def keep_copies(i):
        span = pl.ds(pl.multiple_of(i * 2 * size.lon, 2 * size.lon), 2 * size.lon)
        for k, (src, dst, axis) in enumerate(keeps):
            where = (slice(None), span) if axis else (span, slice(None))
            pltpu.make_async_copy(src.at[where], dst.at[where], ksems.at[k]).start()

    @pl.loop(0, size.lat_rows // 2)
    def _(i):
        moved = [
            forward_tile(size, pl.multiple_of((2 * i + u) * size.lon, size.lon), x_ref[2 * i + u],
                         w1, w2, w3, (h1t, s1, h2t, s2, None))
            for u in (0, 1)
        ]
        analyse(size, (ana_hi[...], ana_lo[...]), moved[0], moved[1], 2 * i, outm)
        xm.start(pl.multiple_of(2 * i * size.pairs, 2 * size.pairs), 2 * size.pairs)
        keep_copies(i)

    xc.wait()
    legendre(size, op_hi, op_lo, gotc, backc_ref, True)
    xm.wait()
    legendre(size, op_hi, op_lo, gotm, backm, False)
    x2.start()
    x2.wait()

    def put(lat, value):
        q_ref[lat] = value

    synthesise(size, (syn_hi[...], syn_lo[...]), got2m, put)
    for x in (xc, xm, x2):
        x.drain()
    for k, (src, dst, _) in enumerate(keeps):
        pltpu.make_async_copy(src, dst, ksems.at[k]).wait()


def plain_dot(a, b):
    return jnp.dot(a, b, preferred_element_type=jnp.float32)


def last_gradient(size, h2t, gt, put):
    half = size.hidden // 2
    for top in (0, half):
        put(size.hidden // LANES * CHUNK + top, plain_dot(h2t[pl.ds(top, half), :], gt[...]))


def middle_gradient(size, h1t, ga2, i, put):
    half = size.hidden // 2
    columns = pl.ds(pl.multiple_of(i * 2 * LANES, 2 * LANES), 2 * LANES)
    for top in (0, half):
        part = plain_dot(h1t[pl.ds(top, half), :], ga2[:, columns])
        for u in (0, 1):
            put(pl.multiple_of((2 * i + u) * CHUNK + top, half), part[:, u * LANES:(u + 1) * LANES])


def first_gradient(size, xt, ga1, put):
    blocks = size.hidden // LANES
    for i in range(blocks // 2):
        part = plain_dot(xt[...], ga1[:, pl.ds(i * 2 * LANES, 2 * LANES)])
        for u in (0, 1):
            put((blocks + 1) * CHUNK + (2 * i + u) * LANES, part[:, u * LANES:(u + 1) * LANES])


def weight_gradients(size, h1t, h2t, xt, gt, ga1, ga2, put):
    last_gradient(size, h2t, gt, put)

    @pl.loop(0, size.hidden // LANES // 2)
    def _(i):
        middle_gradient(size, h1t, ga2, i, put)

    first_gradient(size, xt, ga1, put)


def middle_kernel(size, q_ref, backc_ref, w1, w2, w3, table_hbm, quad,
                  ana_hi, ana_lo, syt_hi, syt_lo, ant_hi, ant_lo,
                  p_ref, backm_ref, g_hbm,
                  table, op_hi, op_lo, h1t, s1, h2t, s2, xt, pulled, gt, ga1, ga2, g,
                  got2c, outm, gotm, outg, gotg, backg, got2g, tsem, gsem, *sems):
    x2c = Exchange(size, backc_ref, got2c, *sems[0:2])
    xm = Exchange(size, outm, gotm, *sems[2:4])
    xg = Exchange(size, outg, gotg, *sems[4:6])
    x2g = Exchange(size, backg, got2g, *sems[6:8])
    greet_lat(size)
    table_in = table_copy(size, table_hbm, table, tsem)
    table_in.start()
    greeted(size.bands - 1)
    x2c.start()
    table_in.wait()
    build_operator(size, table, quad, op_hi, op_lo)

    @pl.loop(0, size.lat_rows // 2)
    def _(i):
        moved = [
            forward_tile(size, pl.multiple_of((2 * i + u) * size.lon, size.lon), q_ref[2 * i + u],
                         w1, w2, w3, (h1t, s1, h2t, s2, xt))
            for u in (0, 1)
        ]
        analyse(size, (ana_hi[...], ana_lo[...]), moved[0], moved[1], 2 * i, outm)

    x2c.wait()

    def put(lat, value):
        pulled[lat] = value

    synthesise(size, (ant_hi[...], ant_lo[...]), got2c, put)
    xm.start()

    @pl.loop(0, size.lat_rows // 2)
    def _(i):
        span = pl.ds(pl.multiple_of(2 * i * size.lon, 2 * size.lon), 2 * size.lon)
        p = jnp.concatenate([pulled[2 * i], pulled[2 * i + 1]], axis=0)
        g_t = (tend_weight * p).astype(jnp.bfloat16)
        gt[span, :] = g_t
        g_a2 = (mul_t(g_t, w3[...]) * s2[span, :].astype(jnp.float32)).astype(jnp.bfloat16)
        ga2[span, :] = g_a2
        g_a1 = (mul_t(g_a2, w2[...]) * s1[span, :].astype(jnp.float32)).astype(jnp.bfloat16)
        ga1[span, :] = g_a1
        grad = p + mul_t(g_a1, w1[...])
        analyse(size, (syt_hi[...], syt_lo[...]), grad[:size.lon], grad[size.lon:], 2 * i, outg)
        xg.start(pl.multiple_of(2 * i * size.pairs, 2 * size.pairs), 2 * size.pairs)

    def keep(row, value):
        g[pl.ds(row, value.shape[0]), :] = value

    weight_gradients(size, h1t, h2t, xt, gt, ga1, ga2, keep)
    xm.wait()
    legendre(size, op_hi, op_lo, gotm, backm_ref, False)
    g_out = pltpu.make_async_copy(g, g_hbm, gsem)
    g_out.start()
    xg.wait()
    legendre(size, op_hi, op_lo, gotg, backg, True)
    x2g.start()
    x2g.wait()

    def put_pulled(lat, value):
        p_ref[lat] = value

    synthesise(size, (ant_hi[...], ant_lo[...]), got2g, put_pulled)
    for x in (x2c, xm, xg, x2g):
        x.drain()
    g_out.wait()


def last_kernel(size, p_ref, x_ref, backm_ref, w2, w3, syn_hi, syn_lo, g_hbm, h1t_hbm, s1_hbm, h2t_hbm, s2_hbm,
                final_ref, o_hbm, h1t, s1, h2t, s2, xt, gt, ga1, ga2, got2m, lsems, osem, ssem, rsem, *scratch):
    place = Place(size.bands)
    blocks = size.hidden // LANES
    tiles = size.lat_rows // 2
    red = Reduce(place, blocks + 2, scratch)
    g = red.g
    x2m = Exchange(size, backm_ref, got2m, ssem, rsem)
    greet_lat(size)
    signal_to(place.across_core)
    loads = [pltpu.make_async_copy(src, dst, lsems.at[k]) for k, (src, dst) in enumerate(
        ((s2_hbm, s2), (g_hbm, g), (h1t_hbm, h1t), (h2t_hbm, h2t), (s1_hbm, s1)))]
    for load in loads:
        load.start()
    greeted(size.bands)
    x2m.start()
    loads[0].wait()

    def span_of(i):
        return pl.ds(pl.multiple_of(2 * i * size.lon, 2 * size.lon), 2 * size.lon)

    @pl.loop(0, tiles)
    def _(i):
        span = span_of(i)
        g_t = (tend_weight * jnp.concatenate([p_ref[2 * i], p_ref[2 * i + 1]], axis=0)).astype(jnp.bfloat16)
        gt[span, :] = g_t
        ga2[span, :] = (mul_t(g_t, w3[...]) * s2[span, :].astype(jnp.float32)).astype(jnp.bfloat16)

    for load in loads[1:]:
        load.wait()

    def put(row, value):
        g[pl.ds(row, value.shape[0]), :] += value

    middle_gradient(size, h1t, ga2, 0, put)

    @pl.loop(0, red.steps)
    def _(t):
        red.step(t)

        @pl.when(t >= LAGS[-1])
        def _():
            rows = pl.ds(pl.multiple_of((t - LAGS[-1]) * CHUNK, CHUNK), CHUNK)
            pltpu.make_async_copy(red.o.at[rows, :], o_hbm.at[rows, :], osem).start()

        @pl.when(jnp.logical_and(lax.rem(t, 2) == 0, t < blocks - 2))
        def _():
            middle_gradient(size, h1t, ga2, t // 2 + 1, put)

        @pl.when(jnp.logical_and(lax.rem(t, 2) == 1, t < 2 * tiles))
        def _():
            span = span_of(t // 2)
            xt[:, span] = jnp.concatenate([x_ref[t - 1], x_ref[t]], axis=0).astype(jnp.bfloat16).T
            ga1[span, :] = (mul_t(ga2[span, :], w2[...]) * s1[span, :].astype(jnp.float32)).astype(jnp.bfloat16)

        @pl.when(t == blocks - 2)
        def _():
            last_gradient(size, h2t, gt, put)

        @pl.when(t == blocks)
        def _():
            first_gradient(size, xt, ga1, put)

        @pl.when(t == blocks + 2)
        def _():
            x2m.wait()

            def put_final(lat, value):
                final_ref[lat] = value

            synthesise(size, (syn_hi[...], syn_lo[...]), got2m, put_final)

    x2m.drain()
    red.drain()
    pltpu.make_async_copy(red.o, o_hbm, osem).wait()


def unpack_kernel(hidden, features, o_hbm, g1_hbm, g2_hbm, g3_hbm, o, isem, osem):
    blocks = hidden // LANES
    rows = lambda b: pl.ds(b * CHUNK, CHUNK)
    loads = [pltpu.make_async_copy(o_hbm.at[rows(b), :], o.at[rows(b), :], isem.at[b]) for b in range(blocks + 2)]
    stores = [
        pltpu.make_async_copy(o.at[rows(b), :], g2_hbm.at[:, pl.ds(b * LANES, LANES)], osem.at[0])
        for b in range(blocks)
    ] + [pltpu.make_async_copy(o.at[rows(blocks), :], g3_hbm, osem.at[1])]
    firsts = [
        pltpu.make_async_copy(o.at[pl.ds((blocks + 1) * CHUNK + b * features, features), :],
                              g1_hbm.at[:, pl.ds(b * LANES, LANES)], osem.at[2])
        for b in range(blocks)
    ]
    for load in loads:
        load.start()
    for load, store in zip(loads, stores):
        load.wait()
        store.start()
    loads[-1].wait()
    for store in firsts:
        store.start()
    for b, count in enumerate((blocks * CHUNK, CHUNK, CHUNK)):
        pltpu.make_async_copy(o.at[pl.ds(0, count), :], o.at[pl.ds(0, count), :], osem.at[b]).wait()


def fused_body(size, state, cotangent, w1, w2, w3):
    analysis, synthesis = grid_tables(size.lon, MW)
    table, quad = legendre_tables(size.lats, MW)
    pair = lambda t: [jnp.asarray(part) for part in np_halves(t)]
    ana_t, syn_t = pair(analysis.T), pair(synthesis.T)
    ana, syn = pair(analysis), pair(synthesis)
    table, quad = jnp.asarray(table), jnp.asarray(quad)[None, :]
    vmem = pl.BlockSpec(memory_space=pltpu.VMEM)
    hbm = pl.BlockSpec(memory_space=pl.ANY)
    f32, bf16 = jnp.float32, jnp.bfloat16
    field = jax.ShapeDtypeStruct(state.shape[1:], f32)
    blocks = jax.ShapeDtypeStruct((size.bands * size.block, LANES), f32)
    wide = jax.ShapeDtypeStruct((size.rows, size.hidden), bf16)
    tall = jax.ShapeDtypeStruct((size.hidden, size.rows), bf16)
    grads = jax.ShapeDtypeStruct(((size.hidden // LANES + 2) * CHUNK, LANES), f32)
    buf = lambda shape: pltpu.VMEM(shape.shape, shape.dtype)
    dma = pltpu.SemaphoreType.DMA
    operator = [pltpu.VMEM((size.waves, MW, size.lats), f32)] + [
        pltpu.VMEM((size.waves, size.lats, size.lats), bf16)] * 2
    narrow = pltpu.VMEM((size.rows, LANES), bf16)
    x_t = pltpu.VMEM((LANES, size.rows), bf16)
    work = size.rows * size.hidden * (size.hidden + 2 * size.features)
    call = lambda kernel, ident, flops, ins, outs, shapes, scratch: pl.pallas_call(
        functools.partial(kernel, size), in_specs=ins, out_specs=outs, out_shape=shapes, scratch_shapes=scratch,
        cost_estimate=pl.CostEstimate(flops=flops, bytes_accessed=2**24, transcendentals=0),
        compiler_params=pltpu.CompilerParams(
            collective_id=ident, has_side_effects=True, vmem_limit_bytes=60 * 2**20))
    x0 = state[0]
    q1, back_c, *saved = call(
        first_kernel, 1, 2 * work, [vmem] * 5 + [hbm] + [vmem] * 7, [vmem] * 2 + [hbm] * 4,
        [field, blocks, tall, wide, tall, wide],
        operator + [buf(tall), buf(wide), buf(tall), buf(wide)] + [buf(blocks)] * 6
        + [dma, dma((4,))] + Exchange.sems(size) * 3,
    )(x0, cotangent[0], w1, w2, w3, table, quad, *ana_t, *syn_t, *syn)
    pulled0, back_m, sums = call(
        middle_kernel, 2, 6 * work, [vmem] * 5 + [hbm] + [vmem] * 7, [vmem, vmem, hbm],
        [field, blocks, grads],
        operator + [buf(tall), buf(wide), buf(tall), buf(wide), x_t, buf(field), narrow, buf(wide), buf(wide),
                    buf(grads)]
        + [buf(blocks)] * 7 + [dma, dma] + Exchange.sems(size) * 4,
    )(q1, back_c, w1, w2, w3, table, quad, *ana_t, *syn_t, *ana)
    final, totals = call(
        last_kernel, 3, 4 * work, [vmem] * 7 + [hbm] * 5, [vmem, hbm], [field, grads],
        [buf(tall), buf(wide), buf(tall), buf(wide), x_t, narrow, buf(wide), buf(wide), buf(blocks), dma((5,)), dma]
        + Exchange.sems(size) + Reduce.scratch(size.hidden // LANES + 2, size.bands // 4),
    )(pulled0, x0, back_m, w2, w3, *syn, sums, *saved)
    g1, g2, g3 = pl.pallas_call(
        functools.partial(unpack_kernel, size.hidden, size.features),
        in_specs=[hbm], out_specs=[hbm] * 3,
        out_shape=[jax.ShapeDtypeStruct(w.shape, f32) for w in (w1, w2, w3)],
        scratch_shapes=[buf(grads), dma((size.hidden // LANES + 2,)), dma((3,))],
    )(totals)
    return final[None], g1, g2, g3


def np_halves(table):
    hi = table.astype(jnp.bfloat16)
    return hi, (table - hi.astype(np.float32)).astype(jnp.bfloat16)


def fits_fused(size, sample):
    return (sample == 1 and size.lat_rows == 8 and size.pairs == 8 and size.lon % 256 == 0
            and size.lats % LANES == 0 and size.bands % 8 == 0)


def body(state, cotangent, w1, w2, w3):
    sample, lat_rows, lon_count, features = state.shape
    bands = lax.axis_size("lat")
    size = Sizes(bands, lat_rows, lon_count, features, w1.shape[1])
    if fits_fused(size, sample) and fits_reduce(bands, lax.axis_size("dp"), features, w1.shape[1]):
        return fused_body(size, state, cotangent, w1, w2, w3)
    lat_count = lat_rows * bands
    waves = MW // bands
    analysis, synthesis = grid_tables(lon_count, MW)
    table, quad = legendre_tables(lat_count, MW)
    mine = lax.dynamic_slice_in_dim(jnp.asarray(table), lax.axis_index("lat") * waves, waves, axis=0)
    base = jnp.einsum("mki,mkj->mij", mine, mine, precision=lax.Precision.HIGHEST)
    quad = jnp.asarray(quad)
    forward_op = base * quad[None, None, :]
    backward_op = base * quad[None, :, None]

    def spectral(parts):
        sent = []
        for field, first, _, _ in parts:
            wav = jnp.einsum("bjxf,xq->bqjf", field, first, precision=high)
            sent.append(wav.reshape(sample, bands, waves * 2, lat_rows, features))
        sent = jnp.concatenate(sent, axis=0).transpose(1, 0, 2, 3, 4)
        got = lax.all_to_all(sent, "lat", split_axis=0, concat_axis=0, tiled=True)
        got = got.reshape(bands, len(parts), sample, waves, 2, lat_rows, features)
        ops = jnp.stack([p[2] for p in parts]).reshape(len(parts), waves, bands, lat_rows, lat_count)
        got = got.transpose(1, 3, 0, 5, 2, 4, 6).reshape(len(parts), waves, lat_count, -1)
        ops = ops.reshape(len(parts), waves, lat_count, lat_count)
        back = jnp.einsum("smij,smjv->smiv", ops, got, precision=high)
        back = back.reshape(len(parts), waves, bands, lat_rows, sample, 2, features)
        back = back.transpose(2, 0, 4, 1, 5, 3, 6)
        back = lax.all_to_all(back, "lat", split_axis=0, concat_axis=0, tiled=True)
        out = []
        for index, (_, _, _, last) in enumerate(parts):
            piece = back[:, index].transpose(1, 0, 2, 3, 4, 5)
            piece = piece.reshape(sample, MW * 2, lat_rows, features)
            out.append(jnp.einsum("bqjf,xq->bjxf", piece, last, precision=high))
        return out

    flat = lambda field: field.reshape(sample * lat_rows * lon_count, features)
    x0 = flat(state)
    moved0, *saved0 = forward_rows(x0, w1, w2, w3)
    (pulled1,) = spectral([(cotangent, synthesis, backward_op, analysis)])
    (q1,) = spectral([(moved0.reshape(state.shape), analysis, forward_op, synthesis)])
    x1 = flat(q1)
    moved1, *saved1 = forward_rows(x1, w1, w2, w3)
    *totals, grad = backward_rows(flat(pulled1), x1, saved1, w1, w2, w3, None, True)
    (final,) = spectral([(moved1.reshape(state.shape), analysis, forward_op, synthesis)])
    (pulled0,) = spectral([(grad.reshape(state.shape), synthesis, backward_op, analysis)])
    totals = backward_rows(flat(pulled0), x0, saved0, w1, w2, w3, totals, False)
    totals = reduce_totals(totals)
    return (final, *totals)


def solution(mesh):
    field = P("dp", "lat", None, None)
    return jax.shard_map(
        body, mesh=mesh, in_specs=(field, field, P(), P(), P()),
        out_specs=(field, P(), P(), P()), check_vma=False,
    )
```

```python
import functools
import math

import jax
import jax.numpy as jnp
import numpy as np
from jax import lax
from jax.experimental import pallas as pl
from jax.experimental.pallas import tpu as pltpu
from jax.sharding import PartitionSpec as P

MW = 64
STEPS = 2

high = lax.Precision.HIGH
tend_weight = 0.5


def grid_tables(lon_count, wave_count):
    lon_index = np.arange(lon_count)
    wave_index = np.arange(wave_count)
    angle = 2.0 * math.pi * (lon_index[:, None] * wave_index[None, :] % lon_count) / lon_count
    pair = np.stack([np.cos(angle), -np.sin(angle)], axis=2)
    factor = np.where(wave_index == 0, 1.0, 2.0)
    analysis = (pair / lon_count).reshape(lon_count, -1).astype(np.float32)
    synthesis = (pair * factor[None, :, None]).reshape(lon_count, -1).astype(np.float32)
    return analysis, synthesis


def legendre_tables(lat_count, wave_count):
    latitude = -0.5 * math.pi + (np.arange(lat_count) + 0.5) * math.pi / lat_count
    mu, cosine = np.sin(latitude), np.cos(latitude)
    quad_weight = cosine * math.pi / lat_count
    order = np.arange(wave_count, dtype=np.float64)
    steps = np.concatenate([[0.0], 0.5 * np.log((2 * order[1:] + 1) / (2 * order[1:]))])
    diagonal = np.exp(
        0.5 * math.log(0.5) + np.cumsum(steps)[:, None] + order[:, None] * np.log(cosine)[None, :]
    )
    rows = [diagonal]
    previous, current, ratio_prev = np.zeros_like(diagonal), diagonal, np.ones_like(order)
    for offset in range(1, wave_count):
        n = order + offset
        ratio = np.sqrt((4 * n * n - 1) / (n * n - order * order))
        following = ratio[:, None] * (mu[None, :] * current - previous / ratio_prev[:, None])
        previous, current, ratio_prev = current, following, ratio
        rows.append(following)
    table = np.stack(rows, axis=1)
    degree = order[:, None] + np.arange(wave_count)[None, :]
    kept = degree <= wave_count - 1
    damping = np.where(kept, 1.0 / (1.0 + degree * (degree + 1) / (wave_count * (wave_count - 1.0))), 0.0)
    table = np.where(kept[:, :, None], table, 0.0) * np.sqrt(damping)[:, :, None]
    return table.astype(np.float32), quad_weight.astype(np.float32)


def silu_pair(value):
    gate = 0.5 * jnp.tanh(0.5 * value) + 0.5
    hidden = value * gate
    return hidden, gate + hidden - hidden * gate


def forward_kernel(x_ref, w1_ref, w2_ref, w3_ref, moved_ref, h1_ref, s1_ref, h2_ref, s2_ref):
    field = x_ref[...]
    rows = field.astype(jnp.bfloat16)
    h1, s1 = silu_pair(jnp.dot(rows, w1_ref[...], preferred_element_type=jnp.float32))
    h1 = h1.astype(jnp.bfloat16)
    h1_ref[...] = h1
    s1_ref[...] = s1.astype(jnp.bfloat16)
    h2, s2 = silu_pair(jnp.dot(h1, w2_ref[...], preferred_element_type=jnp.float32))
    h2 = h2.astype(jnp.bfloat16)
    h2_ref[...] = h2
    s2_ref[...] = s2.astype(jnp.bfloat16)
    tend = jnp.dot(h2, w3_ref[...], preferred_element_type=jnp.float32)
    moved_ref[...] = field + tend_weight * tend


def forward_rows(x, w1, w2, w3):
    count, features = x.shape
    hidden = w1.shape[1]
    tile = math.gcd(count, 256)
    row = lambda width: pl.BlockSpec((tile, width), lambda i: (i, 0))
    whole = lambda w: pl.BlockSpec(w.shape, lambda i: (0, 0))
    wide = jax.ShapeDtypeStruct((count, hidden), jnp.bfloat16)
    return pl.pallas_call(
        forward_kernel,
        grid=(count // tile,),
        in_specs=[row(features), whole(w1), whole(w2), whole(w3)],
        out_specs=[row(features)] + [row(hidden)] * 4,
        out_shape=[jax.ShapeDtypeStruct(x.shape, jnp.float32)] + [wide] * 4,
        cost_estimate=pl.CostEstimate(
            flops=2 * count * (2 * features * hidden + hidden * hidden),
            bytes_accessed=count * hidden * 8, transcendentals=2 * count * hidden,
        ),
        compiler_params=pltpu.CompilerParams(dimension_semantics=("arbitrary",)),
    )(x, w1, w2, w3)


def mul_t(a, b):
    return lax.dot_general(a, b, (((1,), (1,)), ((), ())), preferred_element_type=jnp.float32)


def t_mul(a, b):
    return lax.dot_general(a, b, (((0,), (0,)), ((), ())), preferred_element_type=jnp.float32)


def backward_kernel(first_call, need_rows, *refs):
    p_ref, x_ref, h1_ref, s1_ref, h2_ref, s2_ref, w1_ref, w2_ref, w3_ref = refs[:9]
    refs = refs[9:]
    if not first_call:
        c1_ref, c2_ref, c3_ref = refs[:3]
        refs = refs[3:]
    g1_ref, g2_ref, g3_ref = refs[:3]

    @pl.when(pl.program_id(0) == 0)
    def _():
        if first_call:
            g1_ref[...] = jnp.zeros_like(g1_ref)
            g2_ref[...] = jnp.zeros_like(g2_ref)
            g3_ref[...] = jnp.zeros_like(g3_ref)
        else:
            g1_ref[...] = c1_ref[...]
            g2_ref[...] = c2_ref[...]
            g3_ref[...] = c3_ref[...]

    pulled = p_ref[...]
    gt = (tend_weight * pulled).astype(jnp.bfloat16)
    g3_ref[...] += t_mul(h2_ref[...], gt)
    ga2 = (mul_t(gt, w3_ref[...]) * s2_ref[...].astype(jnp.float32)).astype(jnp.bfloat16)
    g2_ref[...] += t_mul(h1_ref[...], ga2)
    ga1 = (mul_t(ga2, w2_ref[...]) * s1_ref[...].astype(jnp.float32)).astype(jnp.bfloat16)
    g1_ref[...] += t_mul(x_ref[...].astype(jnp.bfloat16), ga1)
    if need_rows:
        refs[3][...] = pulled + mul_t(ga1, w1_ref[...])


def backward_rows(pulled, x, saved, w1, w2, w3, carry, need_rows):
    count, features = x.shape
    hidden = w1.shape[1]
    tile = math.gcd(count, 512)
    row = lambda width: pl.BlockSpec((tile, width), lambda i: (i, 0))
    whole = lambda w: pl.BlockSpec(w.shape, lambda i: (0, 0))
    out_shape = [jax.ShapeDtypeStruct(w.shape, jnp.float32) for w in (w1, w2, w3)]
    out_specs = [whole(w) for w in (w1, w2, w3)]
    carried = [] if carry is None else list(carry)
    if need_rows:
        out_shape.append(jax.ShapeDtypeStruct(x.shape, jnp.float32))
        out_specs.append(row(features))
    return pl.pallas_call(
        functools.partial(backward_kernel, carry is None, need_rows),
        grid=(count // tile,),
        in_specs=[row(features)] * 2 + [row(hidden)] * 4
        + [whole(w) for w in (w1, w2, w3)] + [whole(c) for c in carried],
        out_specs=out_specs,
        out_shape=out_shape,
        cost_estimate=pl.CostEstimate(
            flops=4 * count * (2 * features * hidden + hidden * hidden),
            bytes_accessed=count * hidden * 8, transcendentals=0,
        ),
        compiler_params=pltpu.CompilerParams(dimension_semantics=("arbitrary",)),
    )(pulled, x, *saved, w1, w2, w3, *carried)


MESH_ID = pl.DeviceIdType.MESH
LANES = 128
CHUNK = 1024
SPAN = CHUNK
HALF = SPAN // 2
EARLY = 3
LAGS = (0, 1, 3, 5, 7, 9, 11, 13, 14)


class Place:
    def __init__(self, bands):
        self.me = lax.axis_index("lat")
        self.core = lax.axis_index("dp")
        self.depth = bands // 4
        self.x = lax.rem(self.me, 2)
        self.y = lax.rem(self.me // 2, 2)
        self.z = self.me // 4
        self.across_core = {"dp": 1 - self.core}
        self.across_x = {"lat": self.me + 1 - 2 * self.x}
        self.across_y = {"lat": self.me + 2 - 4 * self.y}

    def along_z(self, step):
        layer = lax.rem(self.z + step, self.depth)
        return layer, {"lat": layer * 4 + lax.rem(self.me, 4)}


def signal_to(device):
    pl.semaphore_signal(pltpu.get_barrier_semaphore(), inc=1, device_id=device, device_id_type=MESH_ID)


def greet_all(place, bands):
    signal_to(place.across_core)

    @pl.loop(1, bands)
    def _(step):
        signal_to({"lat": lax.rem(place.me + step, bands)})


def send(src, dst, ssem, rsem, device):
    pltpu.make_async_remote_copy(
        src_ref=src, dst_ref=dst, send_sem=ssem, recv_sem=rsem, device_id=device, device_id_type=MESH_ID
    ).start()


def wait_bytes(ref, sem):
    pltpu.make_async_copy(ref, ref, sem).wait()


class Reduce:
    SENDS = 8
    REFS = 15

    @staticmethod
    def scratch(chunks, depth):
        rows = lambda parts: pltpu.VMEM((chunks * SPAN // parts, LANES), jnp.float32)
        sems = lambda *dims: pltpu.SemaphoreType.DMA((chunks,) + dims)
        return [
            rows(1), rows(1), rows(2), rows(4), rows(8),
            pltpu.VMEM((chunks, depth - 1, SPAN // 8 // depth, LANES), jnp.float32),
            sems(), sems(2), sems(2), sems(depth - 1), sems(depth - 1), sems(2), sems(2), sems(),
            pltpu.SemaphoreType.DMA((Reduce.SENDS,)),
        ]

    def __init__(self, place, chunks, refs):
        (self.g, self.o, self.r0, self.r1, self.r2, self.r3,
         self.d0, self.m1, self.m2, self.z3, self.z4, self.m5, self.m6, self.d7, self.sent) = refs
        self.place, self.chunks = place, chunks
        self.piece = SPAN // 16 // place.depth
        p = place
        half = p.core * HALF
        self.first = ((p.across_x, p.x), (p.across_y, p.y))
        self.second = (self.first[1], self.first[0])
        self.quarter = (half, half + HALF // 2)
        self.eighth = tuple(self.quarter[i] + self.first[i][1] * (HALF // 4) for i in (0, 1))
        self.sixteenth = tuple(self.eighth[i] + self.second[i][1] * (HALF // 8) for i in (0, 1))
        self.own = tuple(self.sixteenth[i] + p.z * self.piece for i in (0, 1))

    def rows(self, ref, k, offset, count, span=SPAN):
        return ref.at[pl.ds(pl.multiple_of(k * span + offset, 8), count), :]

    def stage0(self, k):
        other = (1 - self.place.core) * HALF
        send(self.rows(self.g, k, other, HALF), self.rows(self.r0, k, 0, HALF, HALF),
             self.sent.at[0], self.d0.at[k], self.place.across_core)

    def stage1(self, k):
        wait_bytes(self.rows(self.r0, k, 0, HALF, HALF), self.d0.at[k])
        mine = self.rows(self.g, k, self.place.core * HALF, HALF)
        mine[...] += self.rows(self.r0, k, 0, HALF, HALF)[...]
        for i in (0, 1):
            device, bit = self.first[i]
            send(self.rows(self.g, k, self.quarter[i] + (1 - bit) * (HALF // 4), HALF // 4),
                 self.rows(self.r1, k, i * (HALF // 4), HALF // 4, HALF // 2), self.sent.at[1], self.m1.at[k, i], device)

    def stage2(self, k):
        for i in (0, 1):
            got = self.rows(self.r1, k, i * (HALF // 4), HALF // 4, HALF // 2)
            wait_bytes(got, self.m1.at[k, i])
            self.rows(self.g, k, self.eighth[i], HALF // 4)[...] += got[...]
        for i in (0, 1):
            device, bit = self.second[i]
            send(self.rows(self.g, k, self.eighth[i] + (1 - bit) * (HALF // 8), HALF // 8),
                 self.rows(self.r2, k, i * (HALF // 8), HALF // 8, HALF // 4), self.sent.at[2], self.m2.at[k, i], device)

    def stage3(self, k):
        for i in (0, 1):
            got = self.rows(self.r2, k, i * (HALF // 8), HALF // 8, HALF // 4)
            wait_bytes(got, self.m2.at[k, i])
            self.rows(self.g, k, self.sixteenth[i], HALF // 8)[...] += got[...]
        for step in range(1, self.place.depth):
            layer, device = self.place.along_z(step)
            for i in (0, 1):
                send(self.rows(self.g, k, self.sixteenth[i] + layer * self.piece, self.piece),
                     self.r3.at[k, step - 1, pl.ds(i * self.piece, self.piece), :],
                     self.sent.at[3], self.z3.at[k, step - 1], device)

    def stage4(self, k):
        total = [self.rows(self.g, k, self.own[i], self.piece)[...] for i in (0, 1)]
        for step in range(1, self.place.depth):
            wait_bytes(self.r3.at[k, step - 1], self.z3.at[k, step - 1])
            for i in (0, 1):
                total[i] += self.r3[k, step - 1, pl.ds(i * self.piece, self.piece), :]
        for i in (0, 1):
            self.rows(self.o, k, self.own[i], self.piece)[...] = total[i]
        for step in range(1, self.place.depth):
            _, device = self.place.along_z(step)
            for i in (0, 1):
                mine = self.rows(self.o, k, self.own[i], self.piece)
                send(mine, mine, self.sent.at[4], self.z4.at[k, step - 1], device)

    def stage5(self, k):
        for step in range(1, self.place.depth):
            wait_bytes(self.r3.at[k, step - 1], self.z4.at[k, step - 1])
        for i in (0, 1):
            mine = self.rows(self.o, k, self.sixteenth[i], HALF // 8)
            send(mine, mine, self.sent.at[5], self.m5.at[k, i], self.second[i][0])

    def stage6(self, k):
        for i in (0, 1):
            wait_bytes(self.rows(self.r2, k, 0, HALF // 8, HALF // 4), self.m5.at[k, i])
        for i in (0, 1):
            mine = self.rows(self.o, k, self.eighth[i], HALF // 4)
            send(mine, mine, self.sent.at[6], self.m6.at[k, i], self.first[i][0])

    def stage7(self, k):
        for i in (0, 1):
            wait_bytes(self.rows(self.r1, k, 0, HALF // 4, HALF // 2), self.m6.at[k, i])
        mine = self.rows(self.o, k, self.place.core * HALF, HALF)
        send(mine, mine, self.sent.at[7], self.d7.at[k], self.place.across_core)

    def stage8(self, k):
        wait_bytes(self.rows(self.r0, k, 0, HALF, HALF), self.d7.at[k])

    def step(self, t):
        stages = [self.stage0, self.stage1, self.stage2, self.stage3, self.stage4,
                  self.stage5, self.stage6, self.stage7, self.stage8]
        for stage, lag in reversed(list(zip(stages, LAGS))):
            k = t - lag

            @pl.when(jnp.logical_and(k >= 0, k < self.chunks))
            def _(k=k, stage=stage):
                stage(k)

    @property
    def steps(self):
        return self.chunks + LAGS[-1]

    def drain(self):
        counts = [HALF, HALF // 2, HALF // 4, 2 * self.piece * (self.place.depth - 1)]
        counts = counts + counts[::-1]
        for i, count in enumerate(counts):
            wait_bytes(self.g.at[pl.ds(0, count * self.chunks), :], self.sent.at[i])


def fits_reduce(bands, pairs, features, hidden):
    return pairs == 2 and bands % 8 == 0 and bands <= 32 and features == LANES and hidden == CHUNK


def reduce_totals(totals):
    return lax.psum(tuple(totals), ("lat", "dp"))


def split_dot(high_low, value, turned=False):
    hi = value.astype(jnp.bfloat16)
    lo = (value - hi.astype(jnp.float32)).astype(jnp.bfloat16)
    table_hi, table_lo = high_low
    mul = t_mul if turned else lambda a, b: jnp.dot(a, b, preferred_element_type=jnp.float32)
    return mul(table_hi, hi) + (mul(table_hi, lo) + mul(table_lo, hi))


def halves(value):
    hi = value.astype(jnp.bfloat16)
    return hi, (value - hi.astype(jnp.float32)).astype(jnp.bfloat16)


class Sizes:
    def __init__(self, bands, lat_rows, lon, features, hidden):
        self.bands, self.lat_rows, self.lon = bands, lat_rows, lon
        self.features, self.hidden = features, hidden
        self.lats = bands * lat_rows
        self.team = bands // 2
        self.half_lats = self.lats // 2
        self.couples = MW // 2 // self.team
        self.pairs = 4 * self.couples
        self.block = self.pairs * lat_rows
        self.rows = lat_rows * lon
        self.all_pairs = 2 * MW
        self.degrees = (MW + 1 + 7) // 8 * 8


class Exchange:
    @staticmethod
    def sems(size):
        return [pltpu.SemaphoreType.DMA, pltpu.SemaphoreType.DMA((size.team,))]

    def __init__(self, size, out, got, ssem, rsem):
        self.size, self.out, self.got, self.ssem, self.rsem = size, out, got, ssem, rsem
        me = lax.axis_index("lat")
        self.me = lax.rem(me, size.team)
        self.base = me - self.me

    def part(self, ref, band, first, count):
        return ref.at[pl.ds(pl.multiple_of(band * self.size.block + first, 8), count), :]

    def start(self, first=0, count=None):
        count = self.size.block if count is None else count

        @pl.loop(1, self.size.team)
        def _(step):
            to = lax.rem(self.me + step, self.size.team)
            send(self.part(self.out, to, first, count), self.part(self.got, self.me, first, count),
                 self.ssem, self.rsem.at[step], {"lat": self.base + to})

        self.part(self.got, self.me, first, count)[...] = self.part(self.out, self.me, first, count)[...]

    def wait(self):
        @pl.loop(1, self.size.team)
        def _(step):
            wait_bytes(self.part(self.got, 0, 0, self.size.block), self.rsem.at[step])

    def drain(self):
        wait_bytes(self.out.at[pl.ds(0, (self.size.team - 1) * self.size.block), :], self.ssem)


class Swap:
    @staticmethod
    def sems(size):
        return [pltpu.SemaphoreType.DMA((size.couples,)), pltpu.SemaphoreType.DMA((size.couples,))]

    def __init__(self, size, out, got, ssem, rsem):
        self.size, self.out, self.got, self.ssem, self.rsem = size, out, got, ssem, rsem

    def part(self, ref, couple):
        return ref.at[pl.ds(couple * 2 * self.size.degrees, 2 * self.size.degrees), :]

    def start(self, couple):
        send(self.part(self.out, couple), self.part(self.got, couple),
             self.ssem.at[couple], self.rsem.at[couple], {"lat": opposite(self.size)})

    def wait(self, couple):
        wait_bytes(self.part(self.got, couple), self.rsem.at[couple])

    def drain(self, couple):
        wait_bytes(self.part(self.out, couple), self.ssem.at[couple])


def opposite(size):
    return lax.rem(lax.axis_index("lat") + size.team, size.bands)


def greeted(count):
    pl.semaphore_wait(pltpu.get_barrier_semaphore(), count)


def build_tables(size, table_ref, quad_ref, plain_hi, plain_lo, quad_hi, quad_lo):
    north = lax.axis_index("lat") // size.team
    width, lats = 2 * size.half_lats, size.half_lats
    source = lax.broadcasted_iota(jnp.int32, (width, width), 0)
    column = lax.broadcasted_iota(jnp.int32, (width, width), 1)
    first = jnp.where(column >= lats, lats, 0)
    mirrored = 2 * first + (lats - 1) - column
    turn = jnp.where(source == jnp.where(north == 1, mirrored, column), 1.0, 0.0).astype(jnp.bfloat16)
    degree = lax.broadcasted_iota(jnp.int32, (size.degrees, width), 0)
    sign = jnp.where(jnp.logical_and(north == 1, lax.rem(degree, 2) == 1), -1.0, 1.0)
    for i in range(size.couples):
        table = table_ref[i] * sign
        for value, hi_ref, lo_ref in ((table, plain_hi, plain_lo), (table * quad_ref[...], quad_hi, quad_lo)):
            for part, ref in zip(halves(value), (hi_ref, lo_ref)):
                ref[i] = plain_dot(part, turn).astype(jnp.bfloat16)


def half_sums(size, table, got, swap, couples):
    for i in range(size.couples):
        value = jnp.concatenate([
            jnp.concatenate(
                [got[pl.ds(4 * i + 2 * w + p, size.half_lats, stride=size.pairs), :] for p in (0, 1)], axis=1)
            for w in (0, 1)], axis=0)
        coef = split_dot((table[0][i], table[1][i]), value)
        for p in (0, 1):
            swap.out[pl.ds((2 * i + p) * size.degrees, size.degrees), :] = coef[:, p * LANES:(p + 1) * LANES]
        if i < couples:
            swap.start(i)


def from_coefs(size, table, swap, exchange):
    for i in range(size.couples):
        swap.wait(i)
        value = jnp.concatenate([
            swap.out[pl.ds((2 * i + p) * size.degrees, size.degrees), :]
            + swap.got[pl.ds((2 * i + p) * size.degrees, size.degrees), :] for p in (0, 1)], axis=1)
        back = split_dot((table[0][i], table[1][i]), value, True)
        for w in (0, 1):
            for p in (0, 1):
                for d in range(size.team):
                    row = w * size.half_lats + d * size.lat_rows
                    exchange.out[pl.ds(d * size.block + (4 * i + 2 * w + p) * size.lat_rows, size.lat_rows), :] = (
                        back[row:row + size.lat_rows, p * LANES:(p + 1) * LANES])
        exchange.start(4 * i * size.lat_rows, 4 * size.lat_rows)


def analyse(size, high_low, first, second, lat, out):
    wav = split_dot(high_low, jnp.concatenate([first, second], axis=1))
    for u in (0, 1):
        for d in range(size.team):
            out[pl.ds(pl.multiple_of(d * size.block + (lat + u) * size.pairs, 8), size.pairs), :] = (
                wav[d * size.pairs:(d + 1) * size.pairs, u * LANES:(u + 1) * LANES])


def synthesise(size, high_low, got, put):
    for lat in range(0, size.lat_rows, 2):
        value = jnp.concatenate(
            [got[pl.ds(lat + u, size.all_pairs, stride=size.lat_rows), :] for u in (0, 1)], axis=1)
        out = split_dot(high_low, value)
        for u in (0, 1):
            put(lat + u, out[:, u * LANES:(u + 1) * LANES])


def forward_tile(size, row, x, w1, w2, w3, keep):
    h1t, s1_ref, h2t, s2_ref, xt = keep
    rows = x.astype(jnp.bfloat16)
    span = pl.ds(row, size.lon)
    if xt is not None:
        xt[:, span] = rows.T
    h1, s1 = silu_pair(jnp.dot(rows, w1[...], preferred_element_type=jnp.float32))
    h1 = h1.astype(jnp.bfloat16)
    s1_ref[span, :] = s1.astype(jnp.bfloat16)
    h1t[:, span] = h1.T
    h2, s2 = silu_pair(jnp.dot(h1, w2[...], preferred_element_type=jnp.float32))
    h2 = h2.astype(jnp.bfloat16)
    s2_ref[span, :] = s2.astype(jnp.bfloat16)
    h2t[:, span] = h2.T
    return x + tend_weight * jnp.dot(h2, w3[...], preferred_element_type=jnp.float32)


def table_copy(size, table_hbm, table_ref, sem):
    return pltpu.make_async_copy(table_hbm.at[lax.rem(lax.axis_index("lat"), size.team)], table_ref, sem)


def plain_dot(a, b):
    return jnp.dot(a, b, preferred_element_type=jnp.float32)


def last_gradient(size, h2t, gt, put):
    half = size.hidden // 2
    for top in (0, half):
        put(top, plain_dot(h2t[pl.ds(top, half), :], gt[...]))


def middle_gradient(size, h1t, ga2, i, put):
    half = size.hidden // 2
    columns = pl.ds(pl.multiple_of(i * 2 * LANES, 2 * LANES), 2 * LANES)
    for top in (0, half):
        part = plain_dot(h1t[pl.ds(top, half), :], ga2[:, columns])
        for u in (0, 1):
            put(pl.multiple_of((2 * i + u + 1) * CHUNK + top, half), part[:, u * LANES:(u + 1) * LANES])


def first_gradient(size, xt, ga1, put):
    blocks = size.hidden // LANES
    for i in range(blocks // 2):
        part = plain_dot(xt[...], ga1[:, pl.ds(i * 2 * LANES, 2 * LANES)])
        for u in (0, 1):
            put((blocks + 1) * CHUNK + (2 * i + u) * LANES, part[:, u * LANES:(u + 1) * LANES])


def weight_gradients(size, h1t, h2t, xt, gt, ga1, ga2, put):
    last_gradient(size, h2t, gt, put)

    @pl.loop(0, size.hidden // LANES // 2)
    def _(i):
        middle_gradient(size, h1t, ga2, i, put)

    first_gradient(size, xt, ga1, put)


def whole_kernel(size, x_hbm, c_hbm, w1_hbm, w2_hbm, w3_hbm, table_hbm, quad,
                 ana_hi, ana_lo, syt_hi, syt_lo, syn_hi, syn_lo, ant_hi, ant_lo,
                 final_hbm, o_hbm, h1t_hbm, s1_hbm, h2t_hbm, s2_hbm, *scratch):
    (x, c, w1, w2, w3, table, p_hi, p_lo, u_hi, u_lo, h1t, s1, h2t, s2, xt0, xt1, gt, ga1, ga2,
     isems, ksems, lsems, fsem, osem) = scratch[:24]
    scratch = list(scratch[24:])

    def take(count):
        taken = scratch[:count]
        del scratch[:count]
        return taken

    place = Place(size.bands)
    blocks = size.hidden // LANES
    tiles = size.lat_rows // 2
    red = Reduce(place, blocks + 2, take(Reduce.REFS))
    g = red.g
    to_c, to_m0, to_m1, to_g = [Exchange(size, *take(4)) for _ in range(4)]
    fro_c, fro_m0, fro_m1, fro_g = [Exchange(size, *take(4)) for _ in range(4)]
    swap_c, swap_m0, swap_m1, swap_g = [Swap(size, *take(4)) for _ in range(4)]
    plain, quads = (p_hi, p_lo), (u_hi, u_lo)

    greet_all(place, size.bands)
    inputs = [pltpu.make_async_copy(src, dst, isems.at[k]) for k, (src, dst) in enumerate(
        ((c_hbm, c), (x_hbm, x), (w1_hbm, w1), (w2_hbm, w2), (w3_hbm, w3)))]
    inputs.append(table_copy(size, table_hbm, table, isems.at[5]))
    for copy in inputs:
        copy.start()

    def span_of(i):
        return pl.ds(pl.multiple_of(2 * i * size.lon, 2 * size.lon), 2 * size.lon)

    def start_tile(exchange, i):
        exchange.start(pl.multiple_of(2 * i * size.pairs, 2 * size.pairs), 2 * size.pairs)

    def store_in(ref):
        def put(lat, value):
            ref[lat] = value
        return put

    inputs[0].wait()

    @pl.loop(0, tiles)
    def _(i):
        analyse(size, (syt_hi[...], syt_lo[...]), c[2 * i], c[2 * i + 1], 2 * i, to_c.out)

    greeted(size.bands)
    to_c.start()
    for copy in inputs[1:]:
        copy.wait()
    build_tables(size, table, quad, *plain, *quads)
    keeps = ((h1t, h1t_hbm, 1), (s1, s1_hbm, 0), (h2t, h2t_hbm, 1), (s2, s2_hbm, 0))

    def forward(i, xt, exchange):
        moved = [
            forward_tile(size, pl.multiple_of((2 * i + u) * size.lon, size.lon), x[2 * i + u],
                         w1, w2, w3, (h1t, s1, h2t, s2, xt))
            for u in (0, 1)
        ]
        analyse(size, (ana_hi[...], ana_lo[...]), moved[0], moved[1], 2 * i, exchange.out)
        start_tile(exchange, i)

    @pl.loop(0, tiles)
    def _(i):
        @pl.when(i == tiles - 1)
        def _():
            to_c.wait()
            half_sums(size, plain, to_c.got, swap_c, EARLY)

        forward(i, xt0, to_m0)
        for k, (src, dst, axis) in enumerate(keeps):
            where = (slice(None), span_of(i)) if axis else (span_of(i), slice(None))
            pltpu.make_async_copy(src.at[where], dst.at[where], ksems.at[k]).start()

    to_m0.wait()
    half_sums(size, quads, to_m0.got, swap_m0, size.couples)
    for i in range(EARLY, size.couples):
        swap_c.start(i)
    from_coefs(size, plain, swap_m0, fro_m0)
    from_coefs(size, quads, swap_c, fro_c)
    for k, (src, dst, _) in enumerate(keeps):
        pltpu.make_async_copy(src, dst, ksems.at[k]).wait()
    fro_m0.wait()
    synthesise(size, (syn_hi[...], syn_lo[...]), fro_m0.got, store_in(x))

    @pl.loop(0, tiles)
    def _(i):
        forward(i, xt1, to_m1)

    fro_c.wait()
    synthesise(size, (ant_hi[...], ant_lo[...]), fro_c.got, store_in(c))

    @pl.loop(0, tiles)
    def _(i):
        @pl.when(i == 1)
        def _():
            to_m1.wait()
            half_sums(size, quads, to_m1.got, swap_m1, size.couples)

        span = span_of(i)
        p = jnp.concatenate([c[2 * i], c[2 * i + 1]], axis=0)
        g_t = (tend_weight * p).astype(jnp.bfloat16)
        gt[span, :] = g_t
        g_a2 = (mul_t(g_t, w3[...]) * s2[span, :].astype(jnp.float32)).astype(jnp.bfloat16)
        ga2[span, :] = g_a2
        g_a1 = (mul_t(g_a2, w2[...]) * s1[span, :].astype(jnp.float32)).astype(jnp.bfloat16)
        ga1[span, :] = g_a1
        grad = p + mul_t(g_a1, w1[...])
        analyse(size, (syt_hi[...], syt_lo[...]), grad[:size.lon], grad[size.lon:], 2 * i, to_g.out)
        start_tile(to_g, i)

    loads = [pltpu.make_async_copy(src, dst, lsems.at[k]) for k, (dst, src, _) in enumerate(keeps)]
    loads[3].start()
    loads[1].start()

    def keep(row, value):
        g[pl.ds(row, value.shape[0]), :] = value

    to_g.wait()
    half_sums(size, plain, to_g.got, swap_g, size.couples)
    from_coefs(size, plain, swap_m1, fro_m1)
    weight_gradients(size, h1t, h2t, xt1, gt, ga1, ga2, keep)
    loads[2].start()
    loads[0].start()
    fro_m1.wait()
    synthesise(size, (syn_hi[...], syn_lo[...]), fro_m1.got, store_in(x))
    final_copy = pltpu.make_async_copy(x, final_hbm, fsem)
    final_copy.start()
    from_coefs(size, quads, swap_g, fro_g)
    fro_g.wait()
    synthesise(size, (ant_hi[...], ant_lo[...]), fro_g.got, store_in(c))

    @pl.loop(0, tiles)
    def _(i):
        gt[span_of(i), :] = (tend_weight * jnp.concatenate([c[2 * i], c[2 * i + 1]], axis=0)).astype(jnp.bfloat16)

    def put(row, value):
        g[pl.ds(row, value.shape[0]), :] += value

    for load in loads:
        load.wait()
    last_gradient(size, h2t, gt, put)

    @pl.loop(0, red.steps)
    def _(t):
        red.step(t)

        @pl.when(t >= LAGS[-1])
        def _():
            rows = pl.ds(pl.multiple_of((t - LAGS[-1]) * CHUNK, CHUNK), CHUNK)
            pltpu.make_async_copy(red.o.at[rows, :], o_hbm.at[rows, :], osem).start()

        @pl.when(t == 0)
        def _():
            @pl.loop(0, tiles)
            def _(i):
                span = span_of(i)
                ga2[span, :] = (mul_t(gt[span, :], w3[...]) * s2[span, :].astype(jnp.float32)).astype(jnp.bfloat16)

        @pl.when(jnp.logical_and(lax.rem(t, 2) == 0, t < blocks))
        def _():
            middle_gradient(size, h1t, ga2, t // 2, put)

        @pl.when(jnp.logical_and(lax.rem(t, 2) == 1, t < 2 * tiles))
        def _():
            span = span_of(t // 2)
            ga1[span, :] = (mul_t(ga2[span, :], w2[...]) * s1[span, :].astype(jnp.float32)).astype(jnp.bfloat16)

        @pl.when(t == blocks)
        def _():
            first_gradient(size, xt0, ga1, put)

    for exchange in (to_c, to_m0, to_m1, to_g, fro_c, fro_m0, fro_m1, fro_g):
        exchange.drain()
    for swap in (swap_c, swap_m0, swap_m1, swap_g):
        for i in range(size.couples):
            swap.drain(i)
    red.drain()
    final_copy.wait()
    pltpu.make_async_copy(red.o, o_hbm, osem).wait()


def unpack_kernel(hidden, features, f_hbm, o_hbm, final_hbm, g1_hbm, g2_hbm, g3_hbm, f, o, isem, osem):
    blocks = hidden // LANES
    rows = lambda b: pl.ds(b * CHUNK, CHUNK)
    load_f = pltpu.make_async_copy(f_hbm, f, isem.at[blocks + 2])
    loads = [pltpu.make_async_copy(o_hbm.at[rows(b), :], o.at[rows(b), :], isem.at[b]) for b in range(blocks + 2)]
    stores = [pltpu.make_async_copy(o.at[rows(0), :], g3_hbm, osem.at[1])] + [
        pltpu.make_async_copy(o.at[rows(b + 1), :], g2_hbm.at[:, pl.ds(b * LANES, LANES)], osem.at[0])
        for b in range(blocks)
    ]
    firsts = [
        pltpu.make_async_copy(o.at[pl.ds((blocks + 1) * CHUNK + b * features, features), :],
                              g1_hbm.at[:, pl.ds(b * LANES, LANES)], osem.at[2])
        for b in range(blocks)
    ]
    store_f = pltpu.make_async_copy(f, final_hbm, osem.at[3])
    for load in loads:
        load.start()
    load_f.start()
    for load, store in zip(loads, stores):
        load.wait()
        store.start()
    loads[-1].wait()
    for store in firsts:
        store.start()
    load_f.wait()
    store_f.start()
    for b, count in enumerate((blocks * CHUNK, CHUNK, CHUNK)):
        pltpu.make_async_copy(o.at[pl.ds(0, count), :], o.at[pl.ds(0, count), :], osem.at[b]).wait()
    store_f.wait()


def packed_tables(size):
    table, quad = legendre_tables(size.lats, MW)
    lats = size.half_lats
    packed = np.zeros((size.team, size.couples, size.degrees, 2 * lats), np.float32)
    order = []
    for d in range(size.team):
        for i in range(size.couples):
            m = d + size.team * i
            other = MW - 1 - m
            packed[d, i, :MW - m, :lats] = table[m, :MW - m, :lats]
            packed[d, i, MW - m:MW + 1, lats:] = table[other, m::-1, :lats]
            order += [2 * m, 2 * m + 1, 2 * other, 2 * other + 1]
    return packed, np.concatenate([quad[:lats]] * 2)[None, :], np.asarray(order)


def fused_body(size, state, cotangent, w1, w2, w3):
    analysis, synthesis = grid_tables(size.lon, MW)
    table, quad, order = packed_tables(size)
    analysis, synthesis = analysis[:, order], synthesis[:, order]
    pair = lambda t: [jnp.asarray(part) for part in np_halves(t)]
    ana_t, syn_t = pair(analysis.T), pair(synthesis.T)
    ana, syn = pair(analysis), pair(synthesis)
    table, quad = jnp.asarray(table), jnp.asarray(quad)
    vmem = pl.BlockSpec(memory_space=pltpu.VMEM)
    hbm = pl.BlockSpec(memory_space=pl.ANY)
    f32, bf16 = jnp.float32, jnp.bfloat16
    field = jax.ShapeDtypeStruct(state.shape[1:], f32)
    blocks = jax.ShapeDtypeStruct((size.team * size.block, LANES), f32)
    coefs = jax.ShapeDtypeStruct((2 * size.couples * size.degrees, LANES), f32)
    wide = jax.ShapeDtypeStruct((size.rows, size.hidden), bf16)
    tall = jax.ShapeDtypeStruct((size.hidden, size.rows), bf16)
    grads = jax.ShapeDtypeStruct(((size.hidden // LANES + 2) * CHUNK, LANES), f32)
    buf = lambda shape: pltpu.VMEM(shape.shape, shape.dtype)
    dma = pltpu.SemaphoreType.DMA
    packed = (size.couples, size.degrees, 2 * size.half_lats)
    tables = [pltpu.VMEM(packed, f32)] + [pltpu.VMEM(packed, bf16)] * 4
    narrow = pltpu.VMEM((size.rows, LANES), bf16)
    x_t = pltpu.VMEM((LANES, size.rows), bf16)
    work = size.rows * size.hidden * (size.hidden + 2 * size.features)
    final, totals, *_ = pl.pallas_call(
        functools.partial(whole_kernel, size),
        in_specs=[hbm] * 6 + [vmem] * 9,
        out_specs=[hbm] * 6,
        out_shape=[field, grads, tall, wide, tall, wide],
        scratch_shapes=[buf(field), buf(field), buf(w1), buf(w2), buf(w3)] + tables
        + [buf(tall), buf(wide), buf(tall), buf(wide), x_t, x_t, narrow, buf(wide), buf(wide)]
        + [dma((6,)), dma((4,)), dma((4,)), dma, dma]
        + Reduce.scratch(size.hidden // LANES + 2, size.bands // 4)
        + ([buf(blocks)] * 2 + Exchange.sems(size)) * 8 + ([buf(coefs)] * 2 + Swap.sems(size)) * 4,
        cost_estimate=pl.CostEstimate(flops=12 * work, bytes_accessed=2**25, transcendentals=0),
        compiler_params=pltpu.CompilerParams(
            collective_id=1, has_side_effects=True, vmem_limit_bytes=63 * 2**20),
    )(state[0], cotangent[0], w1, w2, w3, table, quad, *ana_t, *syn_t, *syn, *ana)
    final, *grads_out = pl.pallas_call(
        functools.partial(unpack_kernel, size.hidden, size.features),
        in_specs=[hbm] * 2, out_specs=[hbm] * 4,
        out_shape=[field] + [jax.ShapeDtypeStruct(w.shape, f32) for w in (w1, w2, w3)],
        scratch_shapes=[buf(field), buf(grads), dma((size.hidden // LANES + 3,)), dma((4,))],
    )(final, totals)
    return (final[None], *grads_out)


def np_halves(table):
    hi = table.astype(jnp.bfloat16)
    return hi, (table - hi.astype(np.float32)).astype(jnp.bfloat16)


def fits_fused(size, sample):
    return (sample == 1 and size.lat_rows == 8 and size.pairs % 8 == 0 and size.lon % 256 == 0
            and size.lats == LANES and size.bands % 8 == 0)


def body(state, cotangent, w1, w2, w3):
    sample, lat_rows, lon_count, features = state.shape
    bands = lax.axis_size("lat")
    size = Sizes(bands, lat_rows, lon_count, features, w1.shape[1])
    if fits_fused(size, sample) and fits_reduce(bands, lax.axis_size("dp"), features, w1.shape[1]):
        return fused_body(size, state, cotangent, w1, w2, w3)
    lat_count = lat_rows * bands
    waves = MW // bands
    analysis, synthesis = grid_tables(lon_count, MW)
    table, quad = legendre_tables(lat_count, MW)
    mine = lax.dynamic_slice_in_dim(jnp.asarray(table), lax.axis_index("lat") * waves, waves, axis=0)
    base = jnp.einsum("mki,mkj->mij", mine, mine, precision=lax.Precision.HIGHEST)
    quad = jnp.asarray(quad)
    forward_op = base * quad[None, None, :]
    backward_op = base * quad[None, :, None]

    def spectral(parts):
        sent = []
        for field, first, _, _ in parts:
            wav = jnp.einsum("bjxf,xq->bqjf", field, first, precision=high)
            sent.append(wav.reshape(sample, bands, waves * 2, lat_rows, features))
        sent = jnp.concatenate(sent, axis=0).transpose(1, 0, 2, 3, 4)
        got = lax.all_to_all(sent, "lat", split_axis=0, concat_axis=0, tiled=True)
        got = got.reshape(bands, len(parts), sample, waves, 2, lat_rows, features)
        ops = jnp.stack([p[2] for p in parts]).reshape(len(parts), waves, bands, lat_rows, lat_count)
        got = got.transpose(1, 3, 0, 5, 2, 4, 6).reshape(len(parts), waves, lat_count, -1)
        ops = ops.reshape(len(parts), waves, lat_count, lat_count)
        back = jnp.einsum("smij,smjv->smiv", ops, got, precision=high)
        back = back.reshape(len(parts), waves, bands, lat_rows, sample, 2, features)
        back = back.transpose(2, 0, 4, 1, 5, 3, 6)
        back = lax.all_to_all(back, "lat", split_axis=0, concat_axis=0, tiled=True)
        out = []
        for index, (_, _, _, last) in enumerate(parts):
            piece = back[:, index].transpose(1, 0, 2, 3, 4, 5)
            piece = piece.reshape(sample, MW * 2, lat_rows, features)
            out.append(jnp.einsum("bqjf,xq->bjxf", piece, last, precision=high))
        return out

    flat = lambda field: field.reshape(sample * lat_rows * lon_count, features)
    x0 = flat(state)
    moved0, *saved0 = forward_rows(x0, w1, w2, w3)
    (pulled1,) = spectral([(cotangent, synthesis, backward_op, analysis)])
    (q1,) = spectral([(moved0.reshape(state.shape), analysis, forward_op, synthesis)])
    x1 = flat(q1)
    moved1, *saved1 = forward_rows(x1, w1, w2, w3)
    *totals, grad = backward_rows(flat(pulled1), x1, saved1, w1, w2, w3, None, True)
    (final,) = spectral([(moved1.reshape(state.shape), analysis, forward_op, synthesis)])
    (pulled0,) = spectral([(grad.reshape(state.shape), synthesis, backward_op, analysis)])
    totals = backward_rows(flat(pulled0), x0, saved0, w1, w2, w3, totals, False)
    totals = reduce_totals(totals)
    return (final, *totals)


def solution(mesh):
    field = P("dp", "lat", None, None)
    return jax.shard_map(
        body, mesh=mesh, in_specs=(field, field, P(), P(), P()),
        out_specs=(field, P(), P(), P()), check_vma=False,
    )
```

```python
import functools
import math

import jax
import jax.numpy as jnp
import numpy as np
from jax import lax
from jax.experimental import pallas as pl
from jax.experimental.pallas import tpu as pltpu
from jax.sharding import PartitionSpec as P

MW = 64
STEPS = 2

high = lax.Precision.HIGH
tend_weight = 0.5


def grid_tables(lon_count, wave_count):
    lon_index = np.arange(lon_count)
    wave_index = np.arange(wave_count)
    angle = 2.0 * math.pi * (lon_index[:, None] * wave_index[None, :] % lon_count) / lon_count
    pair = np.stack([np.cos(angle), -np.sin(angle)], axis=2)
    factor = np.where(wave_index == 0, 1.0, 2.0)
    analysis = (pair / lon_count).reshape(lon_count, -1).astype(np.float32)
    synthesis = (pair * factor[None, :, None]).reshape(lon_count, -1).astype(np.float32)
    return analysis, synthesis


def legendre_tables(lat_count, wave_count):
    latitude = -0.5 * math.pi + (np.arange(lat_count) + 0.5) * math.pi / lat_count
    mu, cosine = np.sin(latitude), np.cos(latitude)
    quad_weight = cosine * math.pi / lat_count
    order = np.arange(wave_count, dtype=np.float64)
    steps = np.concatenate([[0.0], 0.5 * np.log((2 * order[1:] + 1) / (2 * order[1:]))])
    diagonal = np.exp(
        0.5 * math.log(0.5) + np.cumsum(steps)[:, None] + order[:, None] * np.log(cosine)[None, :]
    )
    rows = [diagonal]
    previous, current, ratio_prev = np.zeros_like(diagonal), diagonal, np.ones_like(order)
    for offset in range(1, wave_count):
        n = order + offset
        ratio = np.sqrt((4 * n * n - 1) / (n * n - order * order))
        following = ratio[:, None] * (mu[None, :] * current - previous / ratio_prev[:, None])
        previous, current, ratio_prev = current, following, ratio
        rows.append(following)
    table = np.stack(rows, axis=1)
    degree = order[:, None] + np.arange(wave_count)[None, :]
    kept = degree <= wave_count - 1
    damping = np.where(kept, 1.0 / (1.0 + degree * (degree + 1) / (wave_count * (wave_count - 1.0))), 0.0)
    table = np.where(kept[:, :, None], table, 0.0) * np.sqrt(damping)[:, :, None]
    return table.astype(np.float32), quad_weight.astype(np.float32)


def silu_pair(value):
    gate = 0.5 * jnp.tanh(0.5 * value) + 0.5
    hidden = value * gate
    return hidden, gate + hidden - hidden * gate


def forward_kernel(x_ref, w1_ref, w2_ref, w3_ref, moved_ref, h1_ref, s1_ref, h2_ref, s2_ref):
    field = x_ref[...]
    rows = field.astype(jnp.bfloat16)
    h1, s1 = silu_pair(jnp.dot(rows, w1_ref[...], preferred_element_type=jnp.float32))
    h1 = h1.astype(jnp.bfloat16)
    h1_ref[...] = h1
    s1_ref[...] = s1.astype(jnp.bfloat16)
    h2, s2 = silu_pair(jnp.dot(h1, w2_ref[...], preferred_element_type=jnp.float32))
    h2 = h2.astype(jnp.bfloat16)
    h2_ref[...] = h2
    s2_ref[...] = s2.astype(jnp.bfloat16)
    tend = jnp.dot(h2, w3_ref[...], preferred_element_type=jnp.float32)
    moved_ref[...] = field + tend_weight * tend


def forward_rows(x, w1, w2, w3):
    count, features = x.shape
    hidden = w1.shape[1]
    tile = math.gcd(count, 256)
    row = lambda width: pl.BlockSpec((tile, width), lambda i: (i, 0))
    whole = lambda w: pl.BlockSpec(w.shape, lambda i: (0, 0))
    wide = jax.ShapeDtypeStruct((count, hidden), jnp.bfloat16)
    return pl.pallas_call(
        forward_kernel,
        grid=(count // tile,),
        in_specs=[row(features), whole(w1), whole(w2), whole(w3)],
        out_specs=[row(features)] + [row(hidden)] * 4,
        out_shape=[jax.ShapeDtypeStruct(x.shape, jnp.float32)] + [wide] * 4,
        cost_estimate=pl.CostEstimate(
            flops=2 * count * (2 * features * hidden + hidden * hidden),
            bytes_accessed=count * hidden * 8, transcendentals=2 * count * hidden,
        ),
        compiler_params=pltpu.CompilerParams(dimension_semantics=("arbitrary",)),
    )(x, w1, w2, w3)


def mul_t(a, b):
    return lax.dot_general(a, b, (((1,), (1,)), ((), ())), preferred_element_type=jnp.float32)


def t_mul(a, b):
    return lax.dot_general(a, b, (((0,), (0,)), ((), ())), preferred_element_type=jnp.float32)


def backward_kernel(first_call, need_rows, *refs):
    p_ref, x_ref, h1_ref, s1_ref, h2_ref, s2_ref, w1_ref, w2_ref, w3_ref = refs[:9]
    refs = refs[9:]
    if not first_call:
        c1_ref, c2_ref, c3_ref = refs[:3]
        refs = refs[3:]
    g1_ref, g2_ref, g3_ref = refs[:3]

    @pl.when(pl.program_id(0) == 0)
    def _():
        if first_call:
            g1_ref[...] = jnp.zeros_like(g1_ref)
            g2_ref[...] = jnp.zeros_like(g2_ref)
            g3_ref[...] = jnp.zeros_like(g3_ref)
        else:
            g1_ref[...] = c1_ref[...]
            g2_ref[...] = c2_ref[...]
            g3_ref[...] = c3_ref[...]

    pulled = p_ref[...]
    gt = (tend_weight * pulled).astype(jnp.bfloat16)
    g3_ref[...] += t_mul(h2_ref[...], gt)
    ga2 = (mul_t(gt, w3_ref[...]) * s2_ref[...].astype(jnp.float32)).astype(jnp.bfloat16)
    g2_ref[...] += t_mul(h1_ref[...], ga2)
    ga1 = (mul_t(ga2, w2_ref[...]) * s1_ref[...].astype(jnp.float32)).astype(jnp.bfloat16)
    g1_ref[...] += t_mul(x_ref[...].astype(jnp.bfloat16), ga1)
    if need_rows:
        refs[3][...] = pulled + mul_t(ga1, w1_ref[...])


def backward_rows(pulled, x, saved, w1, w2, w3, carry, need_rows):
    count, features = x.shape
    hidden = w1.shape[1]
    tile = math.gcd(count, 512)
    row = lambda width: pl.BlockSpec((tile, width), lambda i: (i, 0))
    whole = lambda w: pl.BlockSpec(w.shape, lambda i: (0, 0))
    out_shape = [jax.ShapeDtypeStruct(w.shape, jnp.float32) for w in (w1, w2, w3)]
    out_specs = [whole(w) for w in (w1, w2, w3)]
    carried = [] if carry is None else list(carry)
    if need_rows:
        out_shape.append(jax.ShapeDtypeStruct(x.shape, jnp.float32))
        out_specs.append(row(features))
    return pl.pallas_call(
        functools.partial(backward_kernel, carry is None, need_rows),
        grid=(count // tile,),
        in_specs=[row(features)] * 2 + [row(hidden)] * 4
        + [whole(w) for w in (w1, w2, w3)] + [whole(c) for c in carried],
        out_specs=out_specs,
        out_shape=out_shape,
        cost_estimate=pl.CostEstimate(
            flops=4 * count * (2 * features * hidden + hidden * hidden),
            bytes_accessed=count * hidden * 8, transcendentals=0,
        ),
        compiler_params=pltpu.CompilerParams(dimension_semantics=("arbitrary",)),
    )(pulled, x, *saved, w1, w2, w3, *carried)


MESH_ID = pl.DeviceIdType.MESH
LANES = 128
CHUNK = 1024
SPAN = CHUNK
HALF = SPAN // 2
EARLY = 3
AHEAD = 2
LAGS = (0, 1, 3, 5, 7, 9, 11, 13, 14)


class Place:
    def __init__(self, bands):
        self.me = lax.axis_index("lat")
        self.core = lax.axis_index("dp")
        self.depth = bands // 4
        self.x = lax.rem(self.me, 2)
        self.y = lax.rem(self.me // 2, 2)
        self.z = self.me // 4
        self.across_core = {"dp": 1 - self.core}
        self.across_x = {"lat": self.me + 1 - 2 * self.x}
        self.across_y = {"lat": self.me + 2 - 4 * self.y}

    def along_z(self, step):
        layer = lax.rem(self.z + step, self.depth)
        return layer, {"lat": layer * 4 + lax.rem(self.me, 4)}


def signal_to(device):
    pl.semaphore_signal(pltpu.get_barrier_semaphore(), inc=1, device_id=device, device_id_type=MESH_ID)


def greet_all(place, bands):
    signal_to(place.across_core)

    @pl.loop(1, bands)
    def _(step):
        signal_to({"lat": lax.rem(place.me + step, bands)})


def send(src, dst, ssem, rsem, device):
    pltpu.make_async_remote_copy(
        src_ref=src, dst_ref=dst, send_sem=ssem, recv_sem=rsem, device_id=device, device_id_type=MESH_ID
    ).start()


def wait_bytes(ref, sem):
    pltpu.make_async_copy(ref, ref, sem).wait()


class Reduce:
    SENDS = 8
    REFS = 15

    @staticmethod
    def scratch(chunks, depth):
        rows = lambda parts: pltpu.VMEM((chunks * SPAN // parts, LANES), jnp.float32)
        sems = lambda *dims: pltpu.SemaphoreType.DMA((chunks,) + dims)
        return [
            rows(1), rows(1), rows(2), rows(4), rows(8),
            pltpu.VMEM((chunks, depth - 1, SPAN // 8 // depth, LANES), jnp.float32),
            sems(), sems(2), sems(2), sems(depth - 1), sems(depth - 1), sems(2), sems(2), sems(),
            pltpu.SemaphoreType.DMA((Reduce.SENDS,)),
        ]

    def __init__(self, place, chunks, refs):
        (self.g, self.o, self.r0, self.r1, self.r2, self.r3,
         self.d0, self.m1, self.m2, self.z3, self.z4, self.m5, self.m6, self.d7, self.sent) = refs
        self.place, self.chunks = place, chunks
        self.piece = SPAN // 16 // place.depth
        p = place
        half = p.core * HALF
        self.first = ((p.across_x, p.x), (p.across_y, p.y))
        self.second = (self.first[1], self.first[0])
        self.quarter = (half, half + HALF // 2)
        self.eighth = tuple(self.quarter[i] + self.first[i][1] * (HALF // 4) for i in (0, 1))
        self.sixteenth = tuple(self.eighth[i] + self.second[i][1] * (HALF // 8) for i in (0, 1))
        self.own = tuple(self.sixteenth[i] + p.z * self.piece for i in (0, 1))

    def rows(self, ref, k, offset, count, span=SPAN):
        return ref.at[pl.ds(pl.multiple_of(k * span + offset, 8), count), :]

    def stage0(self, k):
        other = (1 - self.place.core) * HALF
        send(self.rows(self.g, k, other, HALF), self.rows(self.r0, k, 0, HALF, HALF),
             self.sent.at[0], self.d0.at[k], self.place.across_core)

    def stage1(self, k):
        wait_bytes(self.rows(self.r0, k, 0, HALF, HALF), self.d0.at[k])
        mine = self.rows(self.g, k, self.place.core * HALF, HALF)
        mine[...] += self.rows(self.r0, k, 0, HALF, HALF)[...]
        for i in (0, 1):
            device, bit = self.first[i]
            send(self.rows(self.g, k, self.quarter[i] + (1 - bit) * (HALF // 4), HALF // 4),
                 self.rows(self.r1, k, i * (HALF // 4), HALF // 4, HALF // 2), self.sent.at[1], self.m1.at[k, i], device)

    def stage2(self, k):
        for i in (0, 1):
            got = self.rows(self.r1, k, i * (HALF // 4), HALF // 4, HALF // 2)
            wait_bytes(got, self.m1.at[k, i])
            self.rows(self.g, k, self.eighth[i], HALF // 4)[...] += got[...]
        for i in (0, 1):
            device, bit = self.second[i]
            send(self.rows(self.g, k, self.eighth[i] + (1 - bit) * (HALF // 8), HALF // 8),
                 self.rows(self.r2, k, i * (HALF // 8), HALF // 8, HALF // 4), self.sent.at[2], self.m2.at[k, i], device)

    def stage3(self, k):
        for i in (0, 1):
            got = self.rows(self.r2, k, i * (HALF // 8), HALF // 8, HALF // 4)
            wait_bytes(got, self.m2.at[k, i])
            self.rows(self.g, k, self.sixteenth[i], HALF // 8)[...] += got[...]
        for step in range(1, self.place.depth):
            layer, device = self.place.along_z(step)
            for i in (0, 1):
                send(self.rows(self.g, k, self.sixteenth[i] + layer * self.piece, self.piece),
                     self.r3.at[k, step - 1, pl.ds(i * self.piece, self.piece), :],
                     self.sent.at[3], self.z3.at[k, step - 1], device)

    def stage4(self, k):
        total = [self.rows(self.g, k, self.own[i], self.piece)[...] for i in (0, 1)]
        for step in range(1, self.place.depth):
            wait_bytes(self.r3.at[k, step - 1], self.z3.at[k, step - 1])
            for i in (0, 1):
                total[i] += self.r3[k, step - 1, pl.ds(i * self.piece, self.piece), :]
        for i in (0, 1):
            self.rows(self.o, k, self.own[i], self.piece)[...] = total[i]
        for step in range(1, self.place.depth):
            _, device = self.place.along_z(step)
            for i in (0, 1):
                mine = self.rows(self.o, k, self.own[i], self.piece)
                send(mine, mine, self.sent.at[4], self.z4.at[k, step - 1], device)

    def stage5(self, k):
        for step in range(1, self.place.depth):
            wait_bytes(self.r3.at[k, step - 1], self.z4.at[k, step - 1])
        for i in (0, 1):
            mine = self.rows(self.o, k, self.sixteenth[i], HALF // 8)
            send(mine, mine, self.sent.at[5], self.m5.at[k, i], self.second[i][0])

    def stage6(self, k):
        for i in (0, 1):
            wait_bytes(self.rows(self.r2, k, 0, HALF // 8, HALF // 4), self.m5.at[k, i])
        for i in (0, 1):
            mine = self.rows(self.o, k, self.eighth[i], HALF // 4)
            send(mine, mine, self.sent.at[6], self.m6.at[k, i], self.first[i][0])

    def stage7(self, k):
        for i in (0, 1):
            wait_bytes(self.rows(self.r1, k, 0, HALF // 4, HALF // 2), self.m6.at[k, i])
        mine = self.rows(self.o, k, self.place.core * HALF, HALF)
        send(mine, mine, self.sent.at[7], self.d7.at[k], self.place.across_core)

    def stage8(self, k):
        wait_bytes(self.rows(self.r0, k, 0, HALF, HALF), self.d7.at[k])

    def step(self, t):
        stages = [self.stage0, self.stage1, self.stage2, self.stage3, self.stage4,
                  self.stage5, self.stage6, self.stage7, self.stage8]
        for stage, lag in reversed(list(zip(stages, LAGS))):
            k = t - lag

            @pl.when(jnp.logical_and(k >= 0, k < self.chunks))
            def _(k=k, stage=stage):
                stage(k)

    @property
    def steps(self):
        return self.chunks + LAGS[-1]

    def drain(self):
        counts = [HALF, HALF // 2, HALF // 4, 2 * self.piece * (self.place.depth - 1)]
        counts = counts + counts[::-1]
        for i, count in enumerate(counts):
            wait_bytes(self.g.at[pl.ds(0, count * self.chunks), :], self.sent.at[i])


def fits_reduce(bands, pairs, features, hidden):
    return pairs == 2 and bands % 8 == 0 and bands <= 32 and features == LANES and hidden == CHUNK


def reduce_totals(totals):
    return lax.psum(tuple(totals), ("lat", "dp"))


def split_dot(high_low, value, turned=False):
    hi = value.astype(jnp.bfloat16)
    lo = (value - hi.astype(jnp.float32)).astype(jnp.bfloat16)
    table_hi, table_lo = high_low
    mul = t_mul if turned else lambda a, b: jnp.dot(a, b, preferred_element_type=jnp.float32)
    return mul(table_hi, hi) + (mul(table_hi, lo) + mul(table_lo, hi))


def halves(value):
    hi = value.astype(jnp.bfloat16)
    return hi, (value - hi.astype(jnp.float32)).astype(jnp.bfloat16)


class Sizes:
    def __init__(self, bands, lat_rows, lon, features, hidden):
        self.bands, self.lat_rows, self.lon = bands, lat_rows, lon
        self.features, self.hidden = features, hidden
        self.lats = bands * lat_rows
        self.team = bands // 2
        self.half_lats = self.lats // 2
        self.couples = MW // 2 // self.team
        self.pairs = 4 * self.couples
        self.block = self.pairs * lat_rows
        self.rows = lat_rows * lon
        self.all_pairs = 2 * MW
        self.degrees = MW


class Exchange:
    @staticmethod
    def sems(size):
        return [pltpu.SemaphoreType.DMA, pltpu.SemaphoreType.DMA((size.team,))]

    def __init__(self, size, out, got, ssem, rsem):
        self.size, self.out, self.got, self.ssem, self.rsem = size, out, got, ssem, rsem
        me = lax.axis_index("lat")
        self.me = lax.rem(me, size.team)
        self.base = me - self.me

    def part(self, ref, band, first, count):
        return ref.at[pl.ds(pl.multiple_of(band * self.size.block + first, 8), count), :]

    def start(self, first=0, count=None):
        count = self.size.block if count is None else count

        @pl.loop(1, self.size.team)
        def _(step):
            to = lax.rem(self.me + step, self.size.team)
            send(self.part(self.out, to, first, count), self.part(self.got, self.me, first, count),
                 self.ssem, self.rsem.at[step], {"lat": self.base + to})

        self.part(self.got, self.me, first, count)[...] = self.part(self.out, self.me, first, count)[...]

    def wait(self):
        @pl.loop(1, self.size.team)
        def _(step):
            wait_bytes(self.part(self.got, 0, 0, self.size.block), self.rsem.at[step])

    def drain(self):
        wait_bytes(self.out.at[pl.ds(0, (self.size.team - 1) * self.size.block), :], self.ssem)


class Swap:
    @staticmethod
    def sems(size):
        return [pltpu.SemaphoreType.DMA((size.couples,)), pltpu.SemaphoreType.DMA((size.couples,))]

    def __init__(self, size, out, got, ssem, rsem):
        self.size, self.out, self.got, self.ssem, self.rsem = size, out, got, ssem, rsem

    def part(self, ref, couple):
        return ref.at[pl.ds(couple * 2 * self.size.degrees, 2 * self.size.degrees), :]

    def start(self, couple):
        send(self.part(self.out, couple), self.part(self.got, couple),
             self.ssem.at[couple], self.rsem.at[couple], {"lat": opposite(self.size)})

    def wait(self, couple):
        wait_bytes(self.part(self.got, couple), self.rsem.at[couple])

    def drain(self, couple):
        wait_bytes(self.part(self.out, couple), self.ssem.at[couple])


def opposite(size):
    return lax.rem(lax.axis_index("lat") + size.team, size.bands)


def greeted(count):
    pl.semaphore_wait(pltpu.get_barrier_semaphore(), count)


def build_tables(size, table_ref, quad_ref, plain_hi, plain_lo, quad_hi, quad_lo):
    north = lax.axis_index("lat") // size.team
    width, lats = 2 * size.half_lats, size.half_lats
    source = lax.broadcasted_iota(jnp.int32, (width, width), 0)
    column = lax.broadcasted_iota(jnp.int32, (width, width), 1)
    first = jnp.where(column >= lats, lats, 0)
    mirrored = 2 * first + (lats - 1) - column
    turn = jnp.where(source == jnp.where(north == 1, mirrored, column), 1.0, 0.0).astype(jnp.bfloat16)
    degree = lax.broadcasted_iota(jnp.int32, (size.degrees, width), 0)
    degree += jnp.where(lax.broadcasted_iota(jnp.int32, (size.degrees, width), 1) >= lats, 1, 0)
    sign = jnp.where(jnp.logical_and(north == 1, lax.rem(degree, 2) == 1), -1.0, 1.0)
    for i in range(size.couples + 1):
        table = table_ref[i] * sign
        for value, hi_ref, lo_ref in ((table, plain_hi, plain_lo), (table * quad_ref[...], quad_hi, quad_lo)):
            for part, ref in zip(halves(value), (hi_ref, lo_ref)):
                ref[i] = plain_dot(part, turn).astype(jnp.bfloat16)


def unit(size, table, couple, part):
    which = size.couples if couple == 0 and part == 1 else couple
    return table[0][which], table[1][which]


def half_sums(size, table, got, swap, couples):
    for i in range(size.couples):
        value = jnp.concatenate([
            jnp.concatenate(
                [got[pl.ds(4 * i + 2 * w + p, size.half_lats, stride=size.pairs), :] for p in (0, 1)], axis=1)
            for w in (0, 1)], axis=0)
        for p in (0, 1):
            swap.out[pl.ds((2 * i + p) * size.degrees, size.degrees), :] = split_dot(
                unit(size, table, i, p), value[:, p * LANES:(p + 1) * LANES])
        if i < couples:
            swap.start(i)


def from_coefs(size, table, swap, exchange, begun):
    for i in range(size.couples):
        swap.wait(i)
        if i + begun < size.couples:
            swap.start(i + begun)
        for p in (0, 1):
            rows = pl.ds((2 * i + p) * size.degrees, size.degrees)
            back = split_dot(unit(size, table, i, p), swap.out[rows, :] + swap.got[rows, :], True)
            for w in (0, 1):
                for d in range(size.team):
                    row = w * size.half_lats + d * size.lat_rows
                    exchange.out[pl.ds(d * size.block + (4 * i + 2 * w + p) * size.lat_rows, size.lat_rows), :] = (
                        back[row:row + size.lat_rows])
        exchange.start(4 * i * size.lat_rows, 4 * size.lat_rows)


def analyse(size, high_low, first, second, lat, out):
    wav = split_dot(high_low, jnp.concatenate([first, second], axis=1))
    for u in (0, 1):
        for d in range(size.team):
            out[pl.ds(pl.multiple_of(d * size.block + (lat + u) * size.pairs, 8), size.pairs), :] = (
                wav[d * size.pairs:(d + 1) * size.pairs, u * LANES:(u + 1) * LANES])


def synthesise(size, high_low, got, put):
    for lat in range(0, size.lat_rows, 2):
        value = jnp.concatenate(
            [got[pl.ds(lat + u, size.all_pairs, stride=size.lat_rows), :] for u in (0, 1)], axis=1)
        out = split_dot(high_low, value)
        for u in (0, 1):
            put(lat + u, out[:, u * LANES:(u + 1) * LANES])


def forward_tile(size, row, x, w1, w2, w3, keep):
    h1t, s1_ref, h2t, s2_ref, xt = keep
    rows = x.astype(jnp.bfloat16)
    span = pl.ds(row, 2 * size.lon)
    if xt is not None:
        xt[:, span] = rows.T
    h1, s1 = silu_pair(jnp.dot(rows, w1[...], preferred_element_type=jnp.float32))
    h1 = h1.astype(jnp.bfloat16)
    s1_ref[span, :] = s1.astype(jnp.bfloat16)
    h1t[:, span] = h1.T
    h2, s2 = silu_pair(jnp.dot(h1, w2[...], preferred_element_type=jnp.float32))
    h2 = h2.astype(jnp.bfloat16)
    s2_ref[span, :] = s2.astype(jnp.bfloat16)
    h2t[:, span] = h2.T
    return x + tend_weight * jnp.dot(h2, w3[...], preferred_element_type=jnp.float32)


def table_copy(size, table_hbm, table_ref, sem):
    return pltpu.make_async_copy(table_hbm.at[lax.rem(lax.axis_index("lat"), size.team)], table_ref, sem)


def plain_dot(a, b):
    return jnp.dot(a, b, preferred_element_type=jnp.float32)


def last_gradient(size, h2t, gt, put):
    half = size.hidden // 2
    for top in (0, half):
        put(top, plain_dot(h2t[pl.ds(top, half), :], gt[...]))


def middle_gradient(size, h1t, ga2, i, put):
    half = size.hidden // 2
    columns = pl.ds(pl.multiple_of(i * 2 * LANES, 2 * LANES), 2 * LANES)
    for top in (0, half):
        part = plain_dot(h1t[pl.ds(top, half), :], ga2[:, columns])
        for u in (0, 1):
            put(pl.multiple_of((2 * i + u + 1) * CHUNK + top, half), part[:, u * LANES:(u + 1) * LANES])


def first_gradient(size, xt, ga1, put):
    blocks = size.hidden // LANES
    for i in range(blocks // 2):
        part = plain_dot(xt[...], ga1[:, pl.ds(i * 2 * LANES, 2 * LANES)])
        for u in (0, 1):
            put((blocks + 1) * CHUNK + (2 * i + u) * LANES, part[:, u * LANES:(u + 1) * LANES])


def weight_gradients(size, h1t, h2t, xt, gt, ga1, ga2, put, between):
    pieces = size.hidden // LANES // 2
    last_gradient(size, h2t, gt, put)
    for part in range(2):
        @pl.loop(part * (pieces // 2), (part + 1) * (pieces // 2))
        def _(i):
            middle_gradient(size, h1t, ga2, i, put)

        between(part)

    first_gradient(size, xt, ga1, put)


def whole_kernel(size, x_hbm, c_hbm, w1_hbm, w2_hbm, w3_hbm, table_hbm, quad,
                 ana_hi, ana_lo, syt_hi, syt_lo, syn_hi, syn_lo, ant_hi, ant_lo,
                 final_hbm, o_hbm, h1t_hbm, s1_hbm, h2t_hbm, s2_hbm, *scratch):
    (x, c, w1, w2, w3, table, p_hi, p_lo, u_hi, u_lo, h1t, s1, h2t, s2, xt0, xt1, gt, ga1, ga2,
     isems, ksems, lsems, fsem, osem) = scratch[:24]
    scratch = list(scratch[24:])

    def take(count):
        taken = scratch[:count]
        del scratch[:count]
        return taken

    place = Place(size.bands)
    blocks = size.hidden // LANES
    tiles = size.lat_rows // 2
    red = Reduce(place, blocks + 2, take(Reduce.REFS))
    g = red.g
    to_c, to_m0, to_m1, to_g = [Exchange(size, *take(4)) for _ in range(4)]
    fro_c, fro_m0, fro_m1, fro_g = [Exchange(size, *take(4)) for _ in range(4)]
    swap_c, swap_m0, swap_m1, swap_g = [Swap(size, *take(4)) for _ in range(4)]
    plain, quads = (p_hi, p_lo), (u_hi, u_lo)

    greet_all(place, size.bands)
    inputs = [pltpu.make_async_copy(src, dst, isems.at[k]) for k, (src, dst) in enumerate(
        ((c_hbm, c), (x_hbm, x), (w1_hbm, w1), (w2_hbm, w2), (w3_hbm, w3)))]
    inputs.append(table_copy(size, table_hbm, table, isems.at[5]))
    for copy in inputs:
        copy.start()

    def span_of(i):
        return pl.ds(pl.multiple_of(2 * i * size.lon, 2 * size.lon), 2 * size.lon)

    def start_tile(exchange, i):
        exchange.start(pl.multiple_of(2 * i * size.pairs, 2 * size.pairs), 2 * size.pairs)

    def store_in(ref):
        def put(lat, value):
            ref[lat] = value
        return put

    inputs[0].wait()

    @pl.loop(0, tiles)
    def _(i):
        analyse(size, (syt_hi[...], syt_lo[...]), c[2 * i], c[2 * i + 1], 2 * i, to_c.out)

    greeted(size.bands)
    to_c.start()
    for copy in inputs[1:]:
        copy.wait()
    build_tables(size, table, quad, *plain, *quads)
    keeps = ((h1t, h1t_hbm, 1), (s1, s1_hbm, 0), (h2t, h2t_hbm, 1), (s2, s2_hbm, 0))

    def forward(i, xt, exchange):
        moved = forward_tile(size, pl.multiple_of(2 * i * size.lon, 2 * size.lon),
                             jnp.concatenate([x[2 * i], x[2 * i + 1]], axis=0),
                             w1, w2, w3, (h1t, s1, h2t, s2, xt))
        analyse(size, (ana_hi[...], ana_lo[...]), moved[:size.lon], moved[size.lon:], 2 * i, exchange.out)
        start_tile(exchange, i)

    @pl.loop(0, tiles)
    def _(i):
        @pl.when(i == tiles - 1)
        def _():
            to_c.wait()
            half_sums(size, plain, to_c.got, swap_c, EARLY)

        forward(i, xt0, to_m0)
        for k, (src, dst, axis) in enumerate(keeps):
            where = (slice(None), span_of(i)) if axis else (span_of(i), slice(None))
            pltpu.make_async_copy(src.at[where], dst.at[where], ksems.at[k]).start()

    to_m0.wait()
    half_sums(size, quads, to_m0.got, swap_m0, AHEAD)
    from_coefs(size, plain, swap_m0, fro_m0, AHEAD)
    from_coefs(size, quads, swap_c, fro_c, EARLY)
    for k, (src, dst, _) in enumerate(keeps):
        pltpu.make_async_copy(src, dst, ksems.at[k]).wait()
    fro_m0.wait()
    synthesise(size, (syn_hi[...], syn_lo[...]), fro_m0.got, store_in(x))

    @pl.loop(0, tiles)
    def _(i):
        forward(i, xt1, to_m1)

    fro_c.wait()
    synthesise(size, (ant_hi[...], ant_lo[...]), fro_c.got, store_in(c))

    @pl.loop(0, tiles)
    def _(i):
        @pl.when(i == 1)
        def _():
            to_m1.wait()
            half_sums(size, quads, to_m1.got, swap_m1, size.couples)

        span = span_of(i)
        p = jnp.concatenate([c[2 * i], c[2 * i + 1]], axis=0)
        g_t = (tend_weight * p).astype(jnp.bfloat16)
        gt[span, :] = g_t
        g_a2 = (mul_t(g_t, w3[...]) * s2[span, :].astype(jnp.float32)).astype(jnp.bfloat16)
        ga2[span, :] = g_a2
        g_a1 = (mul_t(g_a2, w2[...]) * s1[span, :].astype(jnp.float32)).astype(jnp.bfloat16)
        ga1[span, :] = g_a1
        grad = p + mul_t(g_a1, w1[...])
        analyse(size, (syt_hi[...], syt_lo[...]), grad[:size.lon], grad[size.lon:], 2 * i, to_g.out)
        start_tile(to_g, i)

    loads = [pltpu.make_async_copy(src, dst, lsems.at[k]) for k, (dst, src, _) in enumerate(keeps)]
    loads[3].start()
    loads[1].start()

    def keep(row, value):
        g[pl.ds(row, value.shape[0]), :] = value

    to_g.wait()
    half_sums(size, plain, to_g.got, swap_g, AHEAD)
    from_coefs(size, plain, swap_m1, fro_m1, size.couples)
    weight_gradients(size, h1t, h2t, xt1, gt, ga1, ga2, keep, lambda i: swap_g.start(AHEAD + i))
    loads[2].start()
    loads[0].start()
    fro_m1.wait()
    synthesise(size, (syn_hi[...], syn_lo[...]), fro_m1.got, store_in(x))
    final_copy = pltpu.make_async_copy(x, final_hbm, fsem)
    final_copy.start()
    from_coefs(size, quads, swap_g, fro_g, size.couples)
    fro_g.wait()
    synthesise(size, (ant_hi[...], ant_lo[...]), fro_g.got, store_in(c))

    @pl.loop(0, tiles)
    def _(i):
        gt[span_of(i), :] = (tend_weight * jnp.concatenate([c[2 * i], c[2 * i + 1]], axis=0)).astype(jnp.bfloat16)

    def put(row, value):
        g[pl.ds(row, value.shape[0]), :] += value

    for load in loads:
        load.wait()
    last_gradient(size, h2t, gt, put)

    @pl.loop(0, red.steps)
    def _(t):
        red.step(t)

        @pl.when(t >= LAGS[-1])
        def _():
            rows = pl.ds(pl.multiple_of((t - LAGS[-1]) * CHUNK, CHUNK), CHUNK)
            pltpu.make_async_copy(red.o.at[rows, :], o_hbm.at[rows, :], osem).start()

        @pl.when(t < 2)
        def _():
            @pl.loop(t, 1 + t * (blocks // 2 - 1))
            def _(i):
                columns = pl.ds(pl.multiple_of(i * 2 * LANES, 2 * LANES), 2 * LANES)
                ga2[:, columns] = (mul_t(gt[...], w3[columns, :]) * s2[:, columns].astype(jnp.float32)
                                   ).astype(jnp.bfloat16)

        @pl.when(jnp.logical_and(lax.rem(t, 2) == 0, t < blocks))
        def _():
            middle_gradient(size, h1t, ga2, t // 2, put)

        @pl.when(jnp.logical_and(lax.rem(t, 2) == 1, jnp.logical_and(t > 1, t < blocks)))
        def _():
            first = t // 2 - 1

            @pl.loop(first, jnp.where(t == blocks - 1, tiles, first + 1))
            def _(i):
                span = span_of(i)
                ga1[span, :] = (mul_t(ga2[span, :], w2[...]) * s1[span, :].astype(jnp.float32)).astype(jnp.bfloat16)

        @pl.when(t == blocks)
        def _():
            first_gradient(size, xt0, ga1, put)

    for exchange in (to_c, to_m0, to_m1, to_g, fro_c, fro_m0, fro_m1, fro_g):
        exchange.drain()
    for swap in (swap_c, swap_m0, swap_m1, swap_g):
        for i in range(size.couples):
            swap.drain(i)
    red.drain()
    final_copy.wait()
    pltpu.make_async_copy(red.o, o_hbm, osem).wait()


def unpack_kernel(hidden, features, f_hbm, o_hbm, final_hbm, g1_hbm, g2_hbm, g3_hbm, f, o, isem, osem):
    blocks = hidden // LANES
    rows = lambda b: pl.ds(b * CHUNK, CHUNK)
    load_f = pltpu.make_async_copy(f_hbm, f, isem.at[blocks + 2])
    loads = [pltpu.make_async_copy(o_hbm.at[rows(b), :], o.at[rows(b), :], isem.at[b]) for b in range(blocks + 2)]
    stores = [pltpu.make_async_copy(o.at[rows(0), :], g3_hbm, osem.at[1])] + [
        pltpu.make_async_copy(o.at[rows(b + 1), :], g2_hbm.at[:, pl.ds(b * LANES, LANES)], osem.at[0])
        for b in range(blocks)
    ]
    firsts = [
        pltpu.make_async_copy(o.at[pl.ds((blocks + 1) * CHUNK + b * features, features), :],
                              g1_hbm.at[:, pl.ds(b * LANES, LANES)], osem.at[2])
        for b in range(blocks)
    ]
    store_f = pltpu.make_async_copy(f, final_hbm, osem.at[3])
    for load in loads:
        load.start()
    load_f.start()
    for load, store in zip(loads, stores):
        load.wait()
        store.start()
    loads[-1].wait()
    for store in firsts:
        store.start()
    load_f.wait()
    store_f.start()
    for b, count in enumerate((blocks * CHUNK, CHUNK, CHUNK)):
        pltpu.make_async_copy(o.at[pl.ds(0, count), :], o.at[pl.ds(0, count), :], osem.at[b]).wait()
    store_f.wait()


def packed_tables(size):
    table, quad = legendre_tables(size.lats, MW)
    lats = size.half_lats
    packed = np.zeros((size.team, size.couples + 1, size.degrees, 2 * lats), np.float32)
    order = []

    def fill(out, wave, other, rows):
        out[:rows, :lats] = table[wave, :rows, :lats]
        if rows < MW:
            out[rows:, lats:] = table[other, MW - 1 - rows::-1, :lats]

    for d in range(size.team):
        for i in range(size.couples):
            m = d + size.team * i
            if m == 0:
                middle = MW // 2
                fill(packed[d, i], 0, 0, MW)
                fill(packed[d, size.couples], middle, middle, middle)
                order += [0, 2 * middle, 1, 2 * middle + 1]
                continue
            fill(packed[d, i], m, MW - m, MW - m)
            if i == 0:
                packed[d, size.couples] = packed[d, 0]
            order += [2 * m, 2 * m + 1, 2 * (MW - m), 2 * (MW - m) + 1]
    return packed, np.concatenate([quad[:lats]] * 2)[None, :], np.asarray(order)


def fused_body(size, state, cotangent, w1, w2, w3):
    analysis, synthesis = grid_tables(size.lon, MW)
    table, quad, order = packed_tables(size)
    analysis, synthesis = analysis[:, order], synthesis[:, order]
    pair = lambda t: [jnp.asarray(part) for part in np_halves(t)]
    ana_t, syn_t = pair(analysis.T), pair(synthesis.T)
    ana, syn = pair(analysis), pair(synthesis)
    table, quad = jnp.asarray(table), jnp.asarray(quad)
    vmem = pl.BlockSpec(memory_space=pltpu.VMEM)
    hbm = pl.BlockSpec(memory_space=pl.ANY)
    f32, bf16 = jnp.float32, jnp.bfloat16
    field = jax.ShapeDtypeStruct(state.shape[1:], f32)
    blocks = jax.ShapeDtypeStruct((size.team * size.block, LANES), f32)
    coefs = jax.ShapeDtypeStruct((2 * size.couples * size.degrees, LANES), f32)
    wide = jax.ShapeDtypeStruct((size.rows, size.hidden), bf16)
    tall = jax.ShapeDtypeStruct((size.hidden, size.rows), bf16)
    grads = jax.ShapeDtypeStruct(((size.hidden // LANES + 2) * CHUNK, LANES), f32)
    buf = lambda shape: pltpu.VMEM(shape.shape, shape.dtype)
    dma = pltpu.SemaphoreType.DMA
    packed = (size.couples + 1, size.degrees, 2 * size.half_lats)
    tables = [pltpu.VMEM(packed, f32)] + [pltpu.VMEM(packed, bf16)] * 4
    narrow = pltpu.VMEM((size.rows, LANES), bf16)
    x_t = pltpu.VMEM((LANES, size.rows), bf16)
    work = size.rows * size.hidden * (size.hidden + 2 * size.features)
    final, totals, *_ = pl.pallas_call(
        functools.partial(whole_kernel, size),
        in_specs=[hbm] * 6 + [vmem] * 9,
        out_specs=[hbm] * 6,
        out_shape=[field, grads, tall, wide, tall, wide],
        scratch_shapes=[buf(field), buf(field), buf(w1), buf(w2), buf(w3)] + tables
        + [buf(tall), buf(wide), buf(tall), buf(wide), x_t, x_t, narrow, buf(wide), buf(wide)]
        + [dma((6,)), dma((4,)), dma((4,)), dma, dma]
        + Reduce.scratch(size.hidden // LANES + 2, size.bands // 4)
        + ([buf(blocks)] * 2 + Exchange.sems(size)) * 8 + ([buf(coefs)] * 2 + Swap.sems(size)) * 4,
        cost_estimate=pl.CostEstimate(flops=12 * work, bytes_accessed=2**25, transcendentals=0),
        compiler_params=pltpu.CompilerParams(
            collective_id=1, has_side_effects=True, vmem_limit_bytes=63 * 2**20),
    )(state[0], cotangent[0], w1, w2, w3, table, quad, *ana_t, *syn_t, *syn, *ana)
    final, *grads_out = pl.pallas_call(
        functools.partial(unpack_kernel, size.hidden, size.features),
        in_specs=[hbm] * 2, out_specs=[hbm] * 4,
        out_shape=[field] + [jax.ShapeDtypeStruct(w.shape, f32) for w in (w1, w2, w3)],
        scratch_shapes=[buf(field), buf(grads), dma((size.hidden // LANES + 3,)), dma((4,))],
    )(final, totals)
    return (final[None], *grads_out)


def np_halves(table):
    hi = table.astype(jnp.bfloat16)
    return hi, (table - hi.astype(np.float32)).astype(jnp.bfloat16)


def fits_fused(size, sample):
    return (sample == 1 and size.lat_rows == 8 and size.pairs % 8 == 0 and size.lon % 256 == 0
            and size.lats == LANES and size.bands % 8 == 0)


def body(state, cotangent, w1, w2, w3):
    sample, lat_rows, lon_count, features = state.shape
    bands = lax.axis_size("lat")
    size = Sizes(bands, lat_rows, lon_count, features, w1.shape[1])
    if fits_fused(size, sample) and fits_reduce(bands, lax.axis_size("dp"), features, w1.shape[1]):
        return fused_body(size, state, cotangent, w1, w2, w3)
    lat_count = lat_rows * bands
    waves = MW // bands
    analysis, synthesis = grid_tables(lon_count, MW)
    table, quad = legendre_tables(lat_count, MW)
    mine = lax.dynamic_slice_in_dim(jnp.asarray(table), lax.axis_index("lat") * waves, waves, axis=0)
    base = jnp.einsum("mki,mkj->mij", mine, mine, precision=lax.Precision.HIGHEST)
    quad = jnp.asarray(quad)
    forward_op = base * quad[None, None, :]
    backward_op = base * quad[None, :, None]

    def spectral(parts):
        sent = []
        for field, first, _, _ in parts:
            wav = jnp.einsum("bjxf,xq->bqjf", field, first, precision=high)
            sent.append(wav.reshape(sample, bands, waves * 2, lat_rows, features))
        sent = jnp.concatenate(sent, axis=0).transpose(1, 0, 2, 3, 4)
        got = lax.all_to_all(sent, "lat", split_axis=0, concat_axis=0, tiled=True)
        got = got.reshape(bands, len(parts), sample, waves, 2, lat_rows, features)
        ops = jnp.stack([p[2] for p in parts]).reshape(len(parts), waves, bands, lat_rows, lat_count)
        got = got.transpose(1, 3, 0, 5, 2, 4, 6).reshape(len(parts), waves, lat_count, -1)
        ops = ops.reshape(len(parts), waves, lat_count, lat_count)
        back = jnp.einsum("smij,smjv->smiv", ops, got, precision=high)
        back = back.reshape(len(parts), waves, bands, lat_rows, sample, 2, features)
        back = back.transpose(2, 0, 4, 1, 5, 3, 6)
        back = lax.all_to_all(back, "lat", split_axis=0, concat_axis=0, tiled=True)
        out = []
        for index, (_, _, _, last) in enumerate(parts):
            piece = back[:, index].transpose(1, 0, 2, 3, 4, 5)
            piece = piece.reshape(sample, MW * 2, lat_rows, features)
            out.append(jnp.einsum("bqjf,xq->bjxf", piece, last, precision=high))
        return out

    flat = lambda field: field.reshape(sample * lat_rows * lon_count, features)
    x0 = flat(state)
    moved0, *saved0 = forward_rows(x0, w1, w2, w3)
    (pulled1,) = spectral([(cotangent, synthesis, backward_op, analysis)])
    (q1,) = spectral([(moved0.reshape(state.shape), analysis, forward_op, synthesis)])
    x1 = flat(q1)
    moved1, *saved1 = forward_rows(x1, w1, w2, w3)
    *totals, grad = backward_rows(flat(pulled1), x1, saved1, w1, w2, w3, None, True)
    (final,) = spectral([(moved1.reshape(state.shape), analysis, forward_op, synthesis)])
    (pulled0,) = spectral([(grad.reshape(state.shape), synthesis, backward_op, analysis)])
    totals = backward_rows(flat(pulled0), x0, saved0, w1, w2, w3, totals, False)
    totals = reduce_totals(totals)
    return (final, *totals)


def solution(mesh):
    field = P("dp", "lat", None, None)
    return jax.shard_map(
        body, mesh=mesh, in_specs=(field, field, P(), P(), P()),
        out_specs=(field, P(), P(), P()), check_vma=False,
    )
```
